1024 devices in a mesh: wide: 64 (over y, x), narrow: 4 (over z_lo, core), rep: 4 (over z_hi).
Axes of the slice: x: 8, y: 8, z: 8 (z_hi: 4, z_lo: 2; z = z_hi * 2 + z_lo), core: 2. Of those that a mesh axis runs over, the one named last changes fastest.
Arguments:
- queries: bfloat16 [65536, 2048], P(('rep', 'wide'), 'narrow'), parts along dimension 0, may hold values from -20 to 20
- key_rows: bfloat16 [65536, 512], P(('rep', 'wide'), 'narrow'), parts along dimension 0, may hold values from -20 to 20
- value_rows: bfloat16 [65536, 512], P(('rep', 'wide'), 'narrow'), parts along dimension 0, may hold values from -20 to 20
- residual: bfloat16 [65536, 4096], P(('rep', 'wide', 'narrow')), parts along dimension 0, may hold values from -9 to 9
- out_weight: bfloat16 [2048, 4096], P('narrow'), may hold values from -0.125 to 0.125
- norm_gain: bfloat16 [4096], replicated, may hold values from 0.099609375 to 1.8984375
- span_map: int32 [64], replicated, may hold values from 0 to 63, each once
- segments: int32 [256, 128], P(('rep', 'wide')), parts along dimension 0, may hold values from 0 to 8, as said below
- row_owner: int32 [65536, 1], P(('rep', 'wide', 'narrow')), parts along dimension 0, may hold values from 0 to 63; in each aligned block of 64 rows (0 to 63, 64 to 127, ...) at most 2 rows name the same one
Outputs:
- hidden: bfloat16 [65536, 4096], P(('rep', 'wide', 'narrow')), parts along dimension 0
- ffn_in: bfloat16 [256, 4, 64, 2, 4096], P(('rep', 'wide'), 'narrow'), parts along dimension 0
The draws below stay inside these ranges and needn't reach their ends.
There are 4 independent parts, one for each index of `rep`. The reference program is written for one: setup_inputs(seed, part) draws one part's arguments, and reference() takes and returns one part's arrays. A program takes and returns all parts, laid end to end along the dimension named above; an argument that names none is the same for every part. Nothing has to cross between parts.
Inputs may be any that keep to these rules, and one draw needn't show every extreme that they name: `segments`: in each token block the short document numbers start at 0, never fall, and rise by at most one from a row to the next; short rows 0 and 1 lie in the same document; some token block reaches the largest number. `row_owner`: within each aligned block of 64 rows no owner is named by more than 2 rows; in some blocks an owner is named by exactly 2 rows.
All inputs are finite; a program needn't handle non-finite values.
Results may differ from the reference program's by a relative error of at most 0.012.
Values may be sent and summed in bfloat16 or wider, within the bound.
No kernel may reach another device: no remote copies, remote signals or barrier semaphores. Data moves between devices by JAX's collectives and lax.ppermute only.
A program may use at most 64 MiB of HBM per device.

```python
import math
import jax
import jax.numpy as jnp
import numpy as np
from jax import lax

D = 4096
HEAD = 128
QH = 16
KVH = 4
LONG_DEV = 128
SHORT_DEV = 128
TOK_DEV = 256
ROWS_DEV = 64
CAP = 2
TOKENS = 16384
N_WIDE = 64
N_NARROW = 4


def draw_queries(key, part):
    base = 2.0 * jnp.clip(jax.random.normal(jax.random.fold_in(key, 7), (TOKENS, QH * HEAD), jnp.float32), -6.0, 6.0)
    return base.astype(jnp.bfloat16)


def draw_key_rows(key, part):
    base = jnp.clip(jax.random.normal(jax.random.fold_in(key, 9), (TOKENS, KVH * HEAD), jnp.float32), -6.0, 6.0)
    return base.astype(jnp.bfloat16)


def draw_residual(key, part):
    columns = jnp.arange(D, dtype=jnp.float32) / D
    column_scale = jnp.exp(columns * math.log(3.0))[None, :]
    base = 0.3 * column_scale * jnp.clip(jax.random.normal(jax.random.fold_in(key, 15), (TOKENS, D), jnp.float32), -6.0, 6.0)
    return base.astype(jnp.bfloat16)


def draw_segments(key, part):
    wide_count = TOKENS // TOK_DEV
    odds = max(4, SHORT_DEV // 2)
    bound = max(2, SHORT_DEV // 16)
    step = (SHORT_DEV - 2) // bound
    starts = (jax.random.randint(jax.random.fold_in(key, 31), (wide_count, SHORT_DEV), 0, odds) == 0).astype(jnp.int32)
    starts = starts.at[:, :2].set(0)
    places = jnp.arange(SHORT_DEV, dtype=jnp.int32)
    forced = ((places >= 2) & ((places - 2) % step == 0) & ((places - 2) // step < bound)).astype(jnp.int32)
    forced_block = jax.random.randint(jax.random.fold_in(key, 33), (), 0, wide_count)
    selected = (jnp.arange(wide_count, dtype=jnp.int32) == forced_block)[:, None]
    starts = jnp.where(selected, jnp.maximum(starts, forced[None, :]), starts)
    return jnp.minimum(jnp.cumsum(starts, axis=1), bound).astype(jnp.int32)


def block_levels(own_key, shape, pieces, least, top_value):
    gain = 1.0
    for dim, blocks in pieces:
        heights = jax.random.uniform(jax.random.fold_in(jax.random.fold_in(own_key, 6), dim), (blocks,), jnp.float32, least / len(pieces), top_value / len(pieces))
        gain = gain * jnp.repeat(jnp.exp(heights), shape[dim] // blocks).reshape((-1,) + (1,) * (len(shape) - 1 - dim))
    return gain


def deal_out(key, own, number, rows, amount, top, reach, slope):
    ranking = jax.random.permutation(key, amount)
    crowded, ordinary = portions_of(amount, rows * top, reach, slope, True), portions_of(amount, rows * top, reach, slope, False)
    places = jnp.arange(amount)

    def named(tallies, offset_by):
        used = int((tallies > 0).sum())
        fixed = max(1, used // 4)
        moved = fixed + (places - fixed + offset_by * (used - fixed)) % max(1, amount - fixed)
        return jnp.zeros((amount,), jnp.int32).at[ranking[jnp.where(places < fixed, places, moved)]].set(jnp.asarray(tallies, jnp.int32))

    tallies = jnp.where(number % 4 == 0, named(crowded, number // 4), named(ordinary, number - number // 4 - 1))
    mixed = jax.random.permutation(jax.random.fold_in(own, 3), amount)
    giver, taker = mixed[0:amount // 2 * 2:2], mixed[1:amount // 2 * 2:2]
    slack = jnp.minimum(tallies[giver] - 1, reach - tallies[taker]) // 2
    slack = jnp.where((giver == ranking[0]) | (taker == ranking[0]) | (tallies[taker] == 0), 0, jnp.maximum(slack, 0))
    moved = jax.random.randint(jax.random.fold_in(own, 4), (amount // 2,), 0, 1 << 20) % (slack + 1)
    tallies = tallies.at[giver].add(-moved).at[taker].add(moved)
    labels = jnp.searchsorted(jnp.cumsum(tallies), jnp.arange(rows * top), side="right").astype(jnp.int32)
    table = labels.reshape(top, rows).T
    table = table[jax.random.permutation(jax.random.fold_in(own, 1), rows)]
    offset_by = jax.random.randint(jax.random.fold_in(own, 2), (rows, 1), 0, top)
    return jnp.take_along_axis(table, (jnp.arange(top)[None, :] + offset_by) % top, axis=1)


def portions_of(amount, total, most, lean, full):
    weights = [(1 << 20) // math.isqrt(grade ** lean) + 1 for grade in range(1, amount + 1)]
    largest = most if full else min(most, max(-(-total // amount), total * weights[0] // sum(weights)))
    least = 1 if total - largest >= amount - 1 else 0
    counts, rest = [largest] + [least] * (amount - 1), total - largest - least * (amount - 1)
    while rest > 0:
        candidates = [i for i in range(1, amount) if counts[i] < largest] or [i for i in range(1, amount) if counts[i] < most]
        mass, left = sum([weights[i] for i in candidates]), rest
        for i in candidates:
            addition = min(most - counts[i], max(1, left * weights[i] // mass), rest)
            counts[i] = counts[i] + addition
            rest = rest - addition
    return np.array(counts)


def centred(rng, shape, deviation, limit, shards=(), kind=jnp.bfloat16):
    gain = block_levels(rng, shape, shards, -0.22, 0.18) if shards else 1.0
    values = jax.random.normal(rng, shape, jnp.float32) * deviation * gain
    return jnp.minimum(jnp.maximum(values, -limit), limit).astype(kind)


def setup_inputs(seed: int = 0, part: int = 0) -> dict:
    keys = jax.random.split(jax.random.key(seed), 10)
    own_keys = jax.random.split(jax.random.fold_in(keys[9], part), 10)
    queries = draw_queries(jax.random.fold_in(jax.random.fold_in(keys[9], part), 71), part)
    key_rows = draw_key_rows(jax.random.fold_in(jax.random.fold_in(keys[9], part), 71), part)
    value_rows = centred(own_keys[2], (TOKENS, KVH * HEAD), 4.0, 20.0, ((0, 64), (1, 4)))
    residual = draw_residual(jax.random.fold_in(jax.random.fold_in(keys[9], part), 71), part)
    out_weight = centred(keys[4], (QH * HEAD, D), (QH * HEAD) ** -0.5, 0.125, ((0, 4),))
    norm_gain = jnp.clip(1.0 + 0.18 * jax.random.normal(keys[5], (D,), jnp.float32), 0.099609375, 1.8984375).astype(jnp.bfloat16)
    span_map = jax.random.permutation(keys[6], N_WIDE).astype(jnp.int32)
    segments = draw_segments(jax.random.fold_in(jax.random.fold_in(keys[9], part), 71), part)
    row_owner_keys = jax.random.split(jax.random.fold_in(own_keys[8], 1), TOKENS // ROWS_DEV)
    row_owner_turns = jax.random.permutation(jax.random.fold_in(own_keys[8], 3), TOKENS // ROWS_DEV)
    row_owner = jax.vmap(lambda own, number: deal_out(jax.random.fold_in(own_keys[8], 2), own, number, ROWS_DEV, N_WIDE, 1, CAP, 0))(row_owner_keys, row_owner_turns).reshape((TOKENS, 1))
    return {"queries": queries, "key_rows": key_rows, "value_rows": value_rows, "residual": residual, "out_weight": out_weight, "norm_gain": norm_gain, "span_map": span_map, "segments": segments, "row_owner": row_owner}


def attend(scores, visible, vals):
    masked = jnp.where(visible[:, None, None, :], scores, -1e+30)
    row_max = lax.optimization_barrier(jnp.max(masked, axis=-1, keepdims=True))
    weights = jnp.where(visible[:, None, None, :], jnp.exp(masked - row_max), 0.0)
    weight_sum = lax.optimization_barrier(jnp.sum(weights, axis=-1))
    rounded = weights.astype(jnp.bfloat16)
    mixed = jnp.einsum('qgjk,kgd->qgjd', rounded.astype(jnp.float32), vals.astype(jnp.float32))
    return (mixed / weight_sum[..., None]).astype(jnp.bfloat16)

def reference(queries, key_rows, value_rows, residual, out_weight, norm_gain, span_map, segments, row_owner):
    wide_count = TOKENS // TOK_DEV
    group_size = QH // KVH
    score_scale = HEAD ** (-0.5)
    shaped_q = queries.reshape(wide_count, TOK_DEV, KVH, group_size, HEAD)
    shaped_k = key_rows.reshape(wide_count, TOK_DEV, KVH, HEAD)
    shaped_v = value_rows.reshape(wide_count, TOK_DEV, KVH, HEAD)
    long_keys = shaped_k[:, :LONG_DEV].reshape(wide_count * LONG_DEV, KVH, HEAD).astype(jnp.float32)
    long_values = shaped_v[:, :LONG_DEV].reshape(wide_count * LONG_DEV, KVH, HEAD).astype(jnp.float32)
    key_index = jnp.arange(wide_count * LONG_DEV, dtype=jnp.int32)
    key_pos = span_map[key_index // LONG_DEV] * LONG_DEV + key_index % LONG_DEV
    short_index = jnp.arange(SHORT_DEV, dtype=jnp.int32)

    def per_block(inputs):
        block, q_long, q_short, k_short, v_short, documents = inputs
        query_pos = span_map[block] * LONG_DEV + jnp.arange(LONG_DEV, dtype=jnp.int32)
        scores = jnp.einsum('qgjd,kgd->qgjk', q_long.astype(jnp.float32), long_keys) * score_scale
        long_out = attend(scores, key_pos[None, :] <= query_pos[:, None], long_values)
        short_scores = jnp.einsum('qgjd,kgd->qgjk', q_short.astype(jnp.float32), k_short.astype(jnp.float32)) * score_scale
        visible = (documents[None, :] == documents[:, None]) & (short_index[None, :] <= short_index[:, None])
        short_out = attend(short_scores, visible, v_short)
        return jnp.concatenate([long_out, short_out], axis=0).reshape(TOK_DEV, QH * HEAD)
    attended = lax.map(per_block, (jnp.arange(wide_count, dtype=jnp.int32), shaped_q[:, :LONG_DEV], shaped_q[:, LONG_DEV:], shaped_k[:, LONG_DEV:], shaped_v[:, LONG_DEV:], segments))
    attended = attended.reshape(TOKENS, QH * HEAD)
    group_cols = QH * HEAD // N_NARROW
    summed = jnp.zeros((TOKENS, D), jnp.float32)
    for lane in range(N_NARROW):
        product = jnp.dot(attended[:, lane * group_cols:(lane + 1) * group_cols], out_weight[lane * group_cols:(lane + 1) * group_cols], preferred_element_type=jnp.float32)
        summed = summed + lax.optimization_barrier(product.astype(jnp.bfloat16)).astype(jnp.float32)
    hidden = (residual.astype(jnp.float32) + summed).astype(jnp.bfloat16)
    widened = hidden.astype(jnp.float32)
    normed = (widened * lax.rsqrt(lax.optimization_barrier(jnp.mean(widened * widened, axis=1, keepdims=True)) + 1e-05) * norm_gain.astype(jnp.float32)).astype(jnp.bfloat16)
    blocks = TOKENS // ROWS_DEV
    owners = row_owner[:, 0]
    chosen = (owners[:, None] == jnp.arange(N_WIDE, dtype=jnp.int32)[None, :]).astype(jnp.int32).reshape(blocks, ROWS_DEV, N_WIDE)
    earlier = jnp.cumsum(chosen, axis=1) - chosen
    slot_index = lax.optimization_barrier(jnp.sum(earlier * chosen, axis=-1)).reshape(TOKENS)
    block_of = jnp.arange(TOKENS, dtype=jnp.int32) // ROWS_DEV
    source = block_of // N_NARROW
    lane_of = block_of % N_NARROW
    ffn_in = jnp.zeros((N_WIDE, N_NARROW, N_WIDE, CAP, D), jnp.bfloat16).at[owners, lane_of, source, slot_index].set(normed)
    return (hidden, ffn_in)
```

```python
import jax
import jax.numpy as jnp
from jax import lax
from jax.experimental import pallas as pl
from jax.experimental.pallas import tpu as pltpu
from jax.sharding import PartitionSpec as P

HEAD = 128
LONG_DEV = 128
SIDE = 8
HEADS = 4
SCALE = HEAD ** (-0.5)
FAR = -1e30
STATS = 16
QUERY_GROUPS = [
    [(2 * b + j) * SIDE + 2 * a + i for j in range(2) for i in range(2)]
    for b in range(4)
    for a in range(4)
]
KEY_GROUPS = [
    [(2 * b + j) * SIDE + 2 * a + i for b in range(4) for a in range(4)]
    for j in range(2)
    for i in range(2)
]


def dot_nt(a, b):
    return lax.dot_general(a, b, (((1,), (1,)), ((), ())), preferred_element_type=jnp.float32)


def dot_tn(a, b):
    return lax.dot_general(a, b, (((0,), (0,)), ((), ())), preferred_element_type=jnp.float32)


def heads_down(q):
    return jnp.concatenate([q[:, h * HEAD : (h + 1) * HEAD] for h in range(HEADS)], axis=0)


def heads_across(o):
    return jnp.concatenate(
        [o[:, h * HEAD : (h + 1) * HEAD].T for h in range(HEADS)], axis=1
    )


def prep_kernel(q_ref, k_ref, v_ref, seg_ref, kv_out, q_out, short_out):
    kv = jnp.concatenate([k_ref[:LONG_DEV], v_ref[:LONG_DEV]], axis=1)
    for i in range(kv_out.shape[0]):
        kv_out[i] = kv
    q = q_ref[:LONG_DEV]
    for j in range(q_out.shape[0]):
        q_out[j] = q
    qs = heads_down(q_ref[LONG_DEV:])
    k = k_ref[LONG_DEV:]
    v = v_ref[LONG_DEV:]
    n = k.shape[0]
    seg_q = jnp.broadcast_to(seg_ref[...].astype(jnp.float32), (n, n))
    seg_k = seg_q.T
    row = lax.broadcasted_iota(jnp.int32, (n, n), 0)
    col = lax.broadcasted_iota(jnp.int32, (n, n), 1)
    visible = jnp.where((seg_q == seg_k) & (row <= col), 1.0, 0.0)
    visible = jnp.concatenate([visible] * HEADS, axis=1) > 0.5
    s = dot_nt(k, qs) * SCALE
    s = jnp.where(visible, s, FAR)
    top = jnp.max(s, axis=0, keepdims=True)
    w = jnp.where(visible, jnp.exp(s - top), 0.0)
    total = jnp.sum(w, axis=0, keepdims=True)
    o = dot_tn(v, w.astype(jnp.bfloat16)) / total
    short_out[...] = heads_across(o).astype(jnp.bfloat16)


def three_parts(x):
    high = x.astype(jnp.bfloat16).astype(jnp.float32)
    rest = x - high
    middle = rest.astype(jnp.bfloat16).astype(jnp.float32)
    return high, middle, rest - middle


def attend_kernel(wide_ref, span_ref, q_ref, kv_ref, out_ref, top_ref, sum_ref, acc_ref):
    j = pl.program_id(0)
    w = wide_ref[0]
    y = w // SIDE
    x = w % SIDE
    q_span = span_ref[((y // 2) * 2 + j // 2) * SIDE + (x // 2) * 2 + j % 2]
    qs = heads_down(q_ref[0])
    cols = qs.shape[0]
    top_ref[...] = jnp.full(top_ref.shape, FAR, jnp.float32)
    sum_ref[...] = jnp.zeros(sum_ref.shape, jnp.float32)
    acc_ref[...] = jnp.zeros(acc_ref.shape, jnp.float32)
    step = 2
    rows = step * LONG_DEV

    def advance(c, visible):
        k = kv_ref[c * step : (c + 1) * step, :, :HEAD].reshape(rows, HEAD)
        v = kv_ref[c * step : (c + 1) * step, :, HEAD:].reshape(rows, HEAD)
        s = dot_nt(k, qs)
        if visible is not None:
            s = jnp.where(visible, s, FAR)
        old = top_ref[...]
        new = jnp.maximum(old, jnp.max(s, axis=0, keepdims=True))
        p = jnp.exp((s - new) * SCALE)
        if visible is not None:
            p = jnp.where(visible, p, 0.0)
        factor = jnp.exp((old - new) * SCALE)
        top_ref[...] = new
        sum_ref[...] = sum_ref[...] * factor + jnp.sum(p, axis=0, keepdims=True)
        acc_ref[...] = acc_ref[...] * factor + dot_tn(v, p.astype(jnp.bfloat16))

    for c in range(kv_ref.shape[0] // step):
        spans = []
        for i in range(c * step, (c + 1) * step):
            spans.append(span_ref[((i // 4) * 2 + y % 2) * SIDE + (i % 4) * 2 + x % 2])
        low = jnp.minimum(spans[0], spans[1])
        high = jnp.maximum(spans[0], spans[1])

        @pl.when(high < q_span)
        def _(c=c):
            advance(c, None)

        @pl.when((low <= q_span) & (high >= q_span))
        def _(c=c, spans=spans):
            row = lax.broadcasted_iota(jnp.int32, (rows, cols), 0)
            col = lax.broadcasted_iota(jnp.int32, (rows, cols), 1)
            place = row % LONG_DEV
            key_pos = jnp.where(row < LONG_DEV, spans[0], spans[1]) * LONG_DEV + place
            query_pos = q_span * LONG_DEV + col % LONG_DEV
            advance(c, key_pos <= query_pos)

    total = sum_ref[...]
    o = acc_ref[...] / jnp.where(total > 0.0, total, 1.0)
    out_ref[0, :HEAD] = o.astype(jnp.bfloat16)
    parts = (*three_parts(top_ref[...] * SCALE), *three_parts(total))
    row = lax.broadcasted_iota(jnp.int32, (STATS, cols), 0)
    stats = jnp.zeros((STATS, cols), jnp.float32)
    for i, part in enumerate(parts):
        stats = jnp.where(row == i, part, stats)
    out_ref[0, HEAD:] = stats.astype(jnp.bfloat16)


def project_kernel(core_ref, got_ref, short_ref, weight_ref, send_ref, keep_ref, rows_ref):
    half = LONG_DEV // 2

    @pl.when(pl.program_id(0) == 0)
    def _():
        core = core_ref[0]
        tops, sums = [], []
        for j in range(got_ref.shape[0]):
            stats = got_ref[j, HEAD:].astype(jnp.float32)
            tops.append(stats[0:1] + stats[1:2] + stats[2:3])
            sums.append(stats[3:4] + stats[4:5] + stats[5:6])
        top = jnp.maximum(jnp.maximum(tops[0], tops[1]), jnp.maximum(tops[2], tops[3]))
        shares = [s * jnp.exp(t - top) for s, t in zip(sums, tops)]
        total = (shares[0] + shares[1]) + (shares[2] + shares[3])
        o = got_ref[0, :HEAD].astype(jnp.float32) * (shares[0] / total)
        for j in range(1, 4):
            o = o + got_ref[j, :HEAD].astype(jnp.float32) * (shares[j] / total)
        long = heads_across(o).astype(jnp.bfloat16)
        short = short_ref[...]
        for b in range(2):
            at = pl.multiple_of(jnp.where(core == b, 2 * half, 0), half)
            rows_ref[pl.ds(at, half), :] = long[b * half : (b + 1) * half]
            rows_ref[pl.ds(at + half, half), :] = short[b * half : (b + 1) * half]

    product = jnp.dot(rows_ref[...], weight_ref[...], preferred_element_type=jnp.float32)
    rounded = product.astype(jnp.bfloat16)
    send_ref[...] = rounded[: 2 * half]
    keep_ref[...] = rounded[2 * half :]


def pair_kernel(row_ref, keep_ref, got_ref, out_ref):
    out_ref[...] = (
        keep_ref[...].astype(jnp.float32) + got_ref[...].astype(jnp.float32)
    ).astype(jnp.bfloat16)


def route_kernel(
    row_ref, res_ref, keep_ref, got_ref, far_ref, gain_ref, owner_ref, hidden_ref, out_ref, wide_ref
):
    summed = (keep_ref[...].astype(jnp.float32) + got_ref[...].astype(jnp.float32)) + far_ref[
        ...
    ].astype(jnp.float32)
    hidden = (res_ref[...].astype(jnp.float32) + summed).astype(jnp.bfloat16)
    hidden_ref[...] = hidden
    h = hidden.astype(jnp.float32)
    mean = jnp.mean(h * h, axis=1, keepdims=True)
    normed = (h * lax.rsqrt(mean + 1e-05) * gain_ref[...].astype(jnp.float32)).astype(jnp.bfloat16)
    rows = h.shape[0]
    down = jnp.broadcast_to(owner_ref[...].astype(jnp.float32), (rows, HEAD))
    across = down.T[:rows]
    row = lax.broadcasted_iota(jnp.int32, (rows, rows), 0)
    col = lax.broadcasted_iota(jnp.int32, (rows, rows), 1)
    same = (down[:, :rows] == across) & (row < col)
    slot = jnp.sum(jnp.where(same, 1.0, 0.0), axis=0, keepdims=True)
    mine = across == row.astype(jnp.float32)
    owners = rows
    stride = out_ref.shape[0] // owners
    for s in range(2):
        pick = jnp.where(mine & (slot == float(s)), 1.0, 0.0).astype(jnp.bfloat16)
        placed = jnp.dot(pick, normed, preferred_element_type=jnp.float32)
        for t in range(stride // 2):
            wide_ref[pl.ds(2 * t + s, owners, stride=stride), :] = placed[
                :, t * HEAD : (t + 1) * HEAD
            ]
    out_ref[...] = wide_ref[...].astype(jnp.bfloat16)


def exchange(x, groups=None):
    return lax.all_to_all(x, "wide", 0, 0, tiled=True, axis_index_groups=groups)


def on_device(
    queries, key_rows, value_rows, residual, out_weight, norm_gain, span_map, segments, row_owner
):
    wide = lax.axis_index("wide").astype(jnp.int32).reshape(1)
    narrow = lax.axis_index("narrow").astype(jnp.int32).reshape(1)
    core = narrow & 1
    level = lax.shift_right_logical(narrow, jnp.ones_like(narrow))
    bf = jnp.bfloat16
    cols = queries.shape[1]
    width = out_weight.shape[1]
    kv, qs, short = pl.pallas_call(
        prep_kernel,
        out_shape=(
            jax.ShapeDtypeStruct((16, LONG_DEV, 2 * HEAD), bf),
            jax.ShapeDtypeStruct((4, LONG_DEV, cols), bf),
            jax.ShapeDtypeStruct((LONG_DEV, cols), bf),
        ),
        name="prep",
    )(queries, key_rows, value_rows, segments)
    qs = exchange(qs, QUERY_GROUPS)
    kv = exchange(kv, KEY_GROUPS)
    parts = pl.pallas_call(
        attend_kernel,
        grid_spec=pltpu.PrefetchScalarGridSpec(
            num_scalar_prefetch=2,
            grid=(4,),
            in_specs=[
                pl.BlockSpec((1, LONG_DEV, cols), lambda j, w, m: (j, 0, 0)),
                pl.BlockSpec((16, LONG_DEV, 2 * HEAD), lambda j, w, m: (0, 0, 0)),
            ],
            out_specs=pl.BlockSpec((1, HEAD + STATS, cols), lambda j, w, m: (j, 0, 0)),
            scratch_shapes=[
                pltpu.VMEM((1, cols), jnp.float32),
                pltpu.VMEM((1, cols), jnp.float32),
                pltpu.VMEM((HEAD, cols), jnp.float32),
            ],
        ),
        out_shape=jax.ShapeDtypeStruct((4, HEAD + STATS, cols), bf),
        name="attend",
    )(wide, span_map, qs, kv)
    got = exchange(parts, QUERY_GROUPS)
    block = 1024
    send, keep = pl.pallas_call(
        project_kernel,
        grid_spec=pltpu.PrefetchScalarGridSpec(
            num_scalar_prefetch=1,
            grid=(width // block,),
            in_specs=[
                pl.BlockSpec((4, HEAD + STATS, cols), lambda i, c: (0, 0, 0)),
                pl.BlockSpec((LONG_DEV, cols), lambda i, c: (0, 0)),
                pl.BlockSpec((cols, block), lambda i, c: (0, i)),
            ],
            out_specs=[
                pl.BlockSpec((LONG_DEV, block), lambda i, c: (0, i)),
                pl.BlockSpec((LONG_DEV, block), lambda i, c: (0, i)),
            ],
            scratch_shapes=[pltpu.VMEM((2 * LONG_DEV, cols), bf)],
        ),
        out_shape=(
            jax.ShapeDtypeStruct((LONG_DEV, width), bf),
            jax.ShapeDtypeStruct((LONG_DEV, width), bf),
        ),
        name="project",
    )(core, got, short, out_weight)
    near = lax.ppermute(send, "narrow", [(0, 1), (1, 0), (2, 3), (3, 2)])
    rows = residual.shape[0]
    mine = pl.BlockSpec((rows, width), lambda i, r: (r[0], 0))
    whole = pl.BlockSpec((rows, width), lambda i, r: (0, 0))
    pair = pl.pallas_call(
        pair_kernel,
        grid_spec=pltpu.PrefetchScalarGridSpec(
            num_scalar_prefetch=1, grid=(1,), in_specs=[mine, mine], out_specs=whole
        ),
        out_shape=jax.ShapeDtypeStruct((rows, width), bf),
        name="pair",
    )(1 - level, keep, near)
    far = lax.ppermute(pair, "narrow", [(0, 2), (2, 0), (1, 3), (3, 1)])
    owners = 64
    tiles = 2 * width // HEAD
    hidden, outgoing = pl.pallas_call(
        route_kernel,
        grid_spec=pltpu.PrefetchScalarGridSpec(
            num_scalar_prefetch=1,
            grid=(1,),
            in_specs=[
                whole,
                mine,
                mine,
                whole,
                pl.BlockSpec((1, width), lambda i, r: (0, 0)),
                pl.BlockSpec((rows, 1), lambda i, r: (0, 0)),
            ],
            out_specs=[whole, pl.BlockSpec((owners * tiles, HEAD), lambda i, r: (0, 0))],
            scratch_shapes=[pltpu.VMEM((owners * tiles, HEAD), jnp.float32)],
        ),
        out_shape=(
            jax.ShapeDtypeStruct((rows, width), bf),
            jax.ShapeDtypeStruct((owners * tiles, HEAD), bf),
        ),
        name="route",
    )(level, residual, keep, near, far, norm_gain.reshape(1, width), row_owner)
    arrived = exchange(outgoing.reshape(owners, tiles, HEAD))
    arrived = arrived.reshape(owners, tiles // 2, 2, HEAD).transpose(0, 2, 1, 3)
    return (hidden, arrived.reshape(1, 1, owners, 2, width))


def solution(mesh):
    placed = (
        P(("rep", "wide"), "narrow"),
        P(("rep", "wide"), "narrow"),
        P(("rep", "wide"), "narrow"),
        P(("rep", "wide", "narrow"), None),
        P("narrow", None),
        P(),
        P(),
        P(("rep", "wide"), None),
        P(("rep", "wide", "narrow"), None),
    )
    return jax.shard_map(
        on_device,
        mesh=mesh,
        in_specs=placed,
        out_specs=(
            P(("rep", "wide", "narrow"), None),
            P(("rep", "wide"), "narrow", None, None, None),
        ),
        check_vma=False,
    )
```

```python
import jax
import jax.numpy as jnp
from jax import lax
from jax.experimental import pallas as pl
from jax.experimental.pallas import tpu as pltpu
from jax.sharding import PartitionSpec as P

HEAD = 128
LONG_DEV = 128
SIDE = 8
HEADS = 4
SCALE = HEAD ** (-0.5)
FAR = -1e30
STATS = 16
STEP = 4
SCALE2 = SCALE * 1.4426950408889634
QUERY_GROUPS = [
    [(2 * b + j) * SIDE + 2 * a + i for j in range(2) for i in range(2)]
    for b in range(4)
    for a in range(4)
]
KEY_GROUPS = [
    [(2 * b + j) * SIDE + 2 * a + i for b in range(4) for a in range(4)]
    for j in range(2)
    for i in range(2)
]


def dot_nt(a, b):
    return lax.dot_general(a, b, (((1,), (1,)), ((), ())), preferred_element_type=jnp.float32)


def dot_tn(a, b):
    return lax.dot_general(a, b, (((0,), (0,)), ((), ())), preferred_element_type=jnp.float32)


def heads_down(q):
    return jnp.concatenate([q[:, h * HEAD : (h + 1) * HEAD] for h in range(HEADS)], axis=0)


def heads_across(o):
    return jnp.concatenate(
        [o[:, h * HEAD : (h + 1) * HEAD].T for h in range(HEADS)], axis=1
    )


def prep_kernel(q_ref, k_ref, v_ref, kv_out, q_out):
    kv = jnp.concatenate([k_ref[:LONG_DEV], v_ref[:LONG_DEV]], axis=1)
    for i in range(kv_out.shape[0]):
        kv_out[i] = kv
    q = q_ref[:LONG_DEV]
    for j in range(q_out.shape[0]):
        q_out[j] = q


def short_rows(q_ref, k_ref, v_ref, seg_ref):
    qs = heads_down(q_ref[LONG_DEV:])
    k = k_ref[LONG_DEV:]
    v = v_ref[LONG_DEV:]
    n = k.shape[0]
    seg_q = jnp.broadcast_to(seg_ref[...].astype(jnp.float32), (n, n))
    seg_k = seg_q.T
    row = lax.broadcasted_iota(jnp.int32, (n, n), 0)
    col = lax.broadcasted_iota(jnp.int32, (n, n), 1)
    visible = jnp.where((seg_q == seg_k) & (row <= col), 1.0, 0.0)
    visible = jnp.concatenate([visible] * HEADS, axis=1) > 0.5
    s = dot_nt(k, qs) * SCALE
    s = jnp.where(visible, s, FAR)
    top = jnp.max(s, axis=0, keepdims=True)
    w = jnp.where(visible, jnp.exp(s - top), 0.0)
    total = jnp.sum(w, axis=0, keepdims=True)
    o = dot_tn(v, w.astype(jnp.bfloat16)) / total
    return heads_across(o).astype(jnp.bfloat16)


def three_parts(x):
    high = x.astype(jnp.bfloat16).astype(jnp.float32)
    rest = x - high
    middle = rest.astype(jnp.bfloat16).astype(jnp.float32)
    return high, middle, rest - middle


def attend_kernel(
    wide_ref, span_ref, q_ref, kv_ref, out_ref, list_ref, top_ref, sum_ref, acc_ref
):
    j = pl.program_id(0)
    w = wide_ref[0]
    y = w // SIDE
    x = w % SIDE
    q_span = span_ref[((y // 2) * 2 + j // 2) * SIDE + (x // 2) * 2 + j % 2]
    qs = heads_down(q_ref[j])
    cols = qs.shape[0]
    count = jnp.int32(0)
    for i in range(kv_ref.shape[0]):
        span = span_ref[((i // 4) * 2 + y % 2) * SIDE + (i % 4) * 2 + x % 2]
        list_ref[count] = i
        count = count + jnp.where(span < q_span, 1, 0)
    for i in range(STEP):
        list_ref[count + i] = 0
    own = j == (y % 2) * 2 + x % 2

    def block(i):
        return kv_ref[i, :, :HEAD], kv_ref[i, :, HEAD:]

    @pl.when(own)
    def _():
        k, v = block((y // 2) * 4 + x // 2)
        row = lax.broadcasted_iota(jnp.int32, (LONG_DEV, cols), 0)
        col = lax.broadcasted_iota(jnp.int32, (LONG_DEV, cols), 1)
        s = jnp.where(row <= col % LONG_DEV, dot_nt(k, qs), FAR)
        top = jnp.max(s, axis=0, keepdims=True)
        p = jnp.exp2((s - top) * SCALE2)
        top_ref[...] = top
        sum_ref[...] = jnp.sum(p, axis=0, keepdims=True)
        acc_ref[...] = dot_tn(v, p.astype(jnp.bfloat16))

    @pl.when(jnp.logical_not(own))
    def _():
        top_ref[...] = jnp.full(top_ref.shape, FAR, jnp.float32)
        sum_ref[...] = jnp.zeros(sum_ref.shape, jnp.float32)
        acc_ref[...] = jnp.zeros(acc_ref.shape, jnp.float32)

    def advance(t, carry):
        blocks = [block(list_ref[t * STEP + u]) for u in range(STEP)]
        v = jnp.concatenate([b[1] for b in blocks], axis=0)
        s = dot_nt(jnp.concatenate([b[0] for b in blocks], axis=0), qs)
        s = jnp.concatenate(
            [
                jnp.where(t * STEP + u < count, s[u * LONG_DEV : (u + 1) * LONG_DEV], FAR)
                for u in range(STEP)
            ],
            axis=0,
        )
        old = top_ref[...]
        new = jnp.maximum(old, jnp.max(s, axis=0, keepdims=True))
        p = jnp.exp2((s - new) * SCALE2)
        factor = jnp.exp2((old - new) * SCALE2)
        top_ref[...] = new
        sum_ref[...] = sum_ref[...] * factor + jnp.sum(p, axis=0, keepdims=True)
        acc_ref[...] = acc_ref[...] * factor + dot_tn(v, p.astype(jnp.bfloat16))
        return carry

    lax.fori_loop(0, (count + STEP - 1) // STEP, advance, 0)
    total = sum_ref[...]
    o = acc_ref[...] / jnp.where(total > 0.0, total, 1.0)
    out_ref[0, :HEAD] = o.astype(jnp.bfloat16)
    parts = (*three_parts(top_ref[...] * SCALE2), *three_parts(total))
    row = lax.broadcasted_iota(jnp.int32, (STATS, cols), 0)
    stats = jnp.zeros((STATS, cols), jnp.float32)
    for i, part in enumerate(parts):
        stats = jnp.where(row == i, part, stats)
    out_ref[0, HEAD:] = stats.astype(jnp.bfloat16)


def merged_rows(got_ref):
    tops, sums = [], []
    for j in range(got_ref.shape[0]):
        stats = got_ref[j, HEAD:].astype(jnp.float32)
        tops.append(stats[0:1] + stats[1:2] + stats[2:3])
        sums.append(stats[3:4] + stats[4:5] + stats[5:6])
    top = jnp.maximum(jnp.maximum(tops[0], tops[1]), jnp.maximum(tops[2], tops[3]))
    shares = [s * jnp.exp2(t - top) for s, t in zip(sums, tops)]
    total = (shares[0] + shares[1]) + (shares[2] + shares[3])
    o = got_ref[0, :HEAD].astype(jnp.float32) * (shares[0] / total)
    for j in range(1, 4):
        o = o + got_ref[j, :HEAD].astype(jnp.float32) * (shares[j] / total)
    return heads_across(o).astype(jnp.bfloat16)


def projector(make_rows):
    def kernel(core_ref, *refs):
        *inputs, weight_ref, send_ref, keep_ref, rows_ref = refs
        half = rows_ref.shape[0] // 2

        @pl.when(pl.program_id(0) == 0)
        def _():
            made = make_rows(*inputs)
            core = core_ref[0]
            for b in range(2):
                at = pl.multiple_of(jnp.where(core == b, half, 0), half)
                rows_ref[pl.ds(at, half), :] = made[b * half : (b + 1) * half]

        product = jnp.dot(rows_ref[...], weight_ref[...], preferred_element_type=jnp.float32)
        rounded = product.astype(jnp.bfloat16)
        send_ref[...] = rounded[:half]
        keep_ref[...] = rounded[half:]

    return kernel


def project(make_rows, core, inputs, weight, name):
    cols, width = weight.shape
    half = LONG_DEV // 2
    block = 1024
    out = pl.BlockSpec((half, block), lambda i, c: (0, i))
    shape = jax.ShapeDtypeStruct((half, width), jnp.bfloat16)
    return pl.pallas_call(
        projector(make_rows),
        grid_spec=pltpu.PrefetchScalarGridSpec(
            num_scalar_prefetch=1,
            grid=(width // block,),
            in_specs=[
                *[pl.BlockSpec(memory_space=pltpu.VMEM) for _ in inputs],
                pl.BlockSpec((cols, block), lambda i, c: (0, i)),
            ],
            out_specs=[out, out],
            scratch_shapes=[pltpu.VMEM((2 * half, cols), jnp.bfloat16)],
        ),
        out_shape=(shape, shape),
        name=name,
    )(core, *inputs, weight)


def pair_sum(a, b):
    return (a.astype(jnp.float32) + b.astype(jnp.float32)).astype(jnp.bfloat16)


def route_kernel(
    level_ref,
    res_ref,
    keep_ref,
    near_ref,
    far_ref,
    short_ref,
    gain_ref,
    owner_ref,
    hidden_ref,
    out_ref,
    wide_ref,
):
    long = (keep_ref[...].astype(jnp.float32) + near_ref[...].astype(jnp.float32)) + far_ref[
        ...
    ].astype(jnp.float32)
    summed = jnp.where(level_ref[0] == 0, long, short_ref[...])
    hidden = (res_ref[...].astype(jnp.float32) + summed).astype(jnp.bfloat16)
    hidden_ref[...] = hidden
    h = hidden.astype(jnp.float32)
    mean = jnp.mean(h * h, axis=1, keepdims=True)
    normed = (h * lax.rsqrt(mean + 1e-05) * gain_ref[...].astype(jnp.float32)).astype(jnp.bfloat16)
    rows = h.shape[0]
    down = jnp.broadcast_to(owner_ref[...].astype(jnp.float32), (rows, HEAD))
    across = down.T[:rows]
    row = lax.broadcasted_iota(jnp.int32, (rows, rows), 0)
    col = lax.broadcasted_iota(jnp.int32, (rows, rows), 1)
    same = (down[:, :rows] == across) & (row < col)
    slot = jnp.sum(jnp.where(same, 1.0, 0.0), axis=0, keepdims=True)
    mine = across == row.astype(jnp.float32)
    owners = rows
    stride = out_ref.shape[0] // owners
    for s in range(2):
        pick = jnp.where(mine & (slot == float(s)), 1.0, 0.0).astype(jnp.bfloat16)
        placed = jnp.dot(pick, normed, preferred_element_type=jnp.float32)
        for t in range(stride // 2):
            wide_ref[pl.ds(2 * t + s, owners, stride=stride), :] = placed[
                :, t * HEAD : (t + 1) * HEAD
            ]
    out_ref[...] = wide_ref[...].astype(jnp.bfloat16)


def in_vmem(x):
    return pltpu.with_memory_space_constraint(x, pltpu.VMEM)


def exchange(x, groups=None):
    return lax.all_to_all(x, "wide", 0, 0, tiled=True, axis_index_groups=groups)


def on_device(
    queries, key_rows, value_rows, residual, out_weight, norm_gain, span_map, segments, row_owner
):
    wide = lax.axis_index("wide").astype(jnp.int32).reshape(1)
    narrow = lax.axis_index("narrow").astype(jnp.int32).reshape(1)
    core = narrow & 1
    level = lax.shift_right_logical(narrow, jnp.ones_like(narrow))
    bf = jnp.bfloat16
    cols = queries.shape[1]
    width = out_weight.shape[1]
    vmem = pl.BlockSpec(memory_space=pltpu.VMEM)
    kv, qs = pl.pallas_call(
        prep_kernel,
        out_shape=(
            jax.ShapeDtypeStruct((16, LONG_DEV, 2 * HEAD), bf),
            jax.ShapeDtypeStruct((4, LONG_DEV, cols), bf),
        ),
        name="prep",
    )(queries, key_rows, value_rows)
    across = [(0, 1), (1, 0), (2, 3), (3, 2)]
    kv, qs, core_after = lax.optimization_barrier((kv, qs, core))
    kv = exchange(kv, KEY_GROUPS)
    qs = exchange(qs, QUERY_GROUPS)
    send, keep_short = project(
        short_rows, core_after, (queries, key_rows, value_rows, segments), out_weight, "short"
    )
    near_short = lax.ppermute(send, "narrow", across)
    pair_short = pair_sum(keep_short, near_short)
    far_short = lax.ppermute(pair_short, "narrow", [(0, 2), (1, 3)])
    short = (keep_short.astype(jnp.float32) + near_short.astype(jnp.float32)) + far_short.astype(
        jnp.float32
    )
    wide, short = lax.optimization_barrier((wide, short))
    parts = pl.pallas_call(
        attend_kernel,
        grid_spec=pltpu.PrefetchScalarGridSpec(
            num_scalar_prefetch=2,
            grid=(4,),
            in_specs=[vmem, pl.BlockSpec((16, LONG_DEV, 2 * HEAD), lambda j, w, m: (0, 0, 0))],
            out_specs=pl.BlockSpec((1, HEAD + STATS, cols), lambda j, w, m: (j, 0, 0)),
            scratch_shapes=[
                pltpu.SMEM((16 + STEP,), jnp.int32),
                pltpu.VMEM((1, cols), jnp.float32),
                pltpu.VMEM((1, cols), jnp.float32),
                pltpu.VMEM((HEAD, cols), jnp.float32),
            ],
        ),
        out_shape=jax.ShapeDtypeStruct((4, HEAD + STATS, cols), bf),
        name="attend",
    )(wide, span_map, in_vmem(qs), kv)
    got = exchange(parts, QUERY_GROUPS)
    send, keep = project(merged_rows, core, (in_vmem(got),), out_weight, "long")
    near = lax.ppermute(send, "narrow", across)
    far = lax.ppermute(pair_sum(keep, near), "narrow", [(2, 0), (3, 1)])
    rows = residual.shape[0]
    owners = 64
    tiles = 2 * width // HEAD
    hidden, outgoing = pl.pallas_call(
        route_kernel,
        in_specs=[pl.BlockSpec(memory_space=pltpu.SMEM)] + [vmem] * 7,
        out_shape=(
            jax.ShapeDtypeStruct((rows, width), bf),
            jax.ShapeDtypeStruct((owners * tiles, HEAD), bf),
        ),
        scratch_shapes=[pltpu.VMEM((owners * tiles, HEAD), jnp.float32)],
        name="route",
    )(level, residual, keep, in_vmem(near), in_vmem(far), in_vmem(short), norm_gain.reshape(1, width), row_owner)
    arrived = exchange(outgoing.reshape(owners, tiles, HEAD))
    arrived = arrived.reshape(owners, tiles // 2, 2, HEAD).transpose(0, 2, 1, 3)
    return (hidden, arrived.reshape(1, 1, owners, 2, width))


def solution(mesh):
    placed = (
        P(("rep", "wide"), "narrow"),
        P(("rep", "wide"), "narrow"),
        P(("rep", "wide"), "narrow"),
        P(("rep", "wide", "narrow"), None),
        P("narrow", None),
        P(),
        P(),
        P(("rep", "wide"), None),
        P(("rep", "wide", "narrow"), None),
    )
    return jax.shard_map(
        on_device,
        mesh=mesh,
        in_specs=placed,
        out_specs=(
            P(("rep", "wide", "narrow"), None),
            P(("rep", "wide"), "narrow", None, None, None),
        ),
        check_vma=False,
    )
```

```python
import jax
import jax.numpy as jnp
from jax import lax
from jax.experimental import pallas as pl
from jax.experimental.pallas import tpu as pltpu
from jax.sharding import PartitionSpec as P

HEAD = 128
LONG_DEV = 128
SIDE = 8
HEADS = 4
SCALE = HEAD ** (-0.5)
FAR = -1e30
ROOM = pltpu.CompilerParams(vmem_limit_bytes=24 * 1024 * 1024)
STATS = 16
STEP = 4
SCALE2 = SCALE * 1.4426950408889634
QUERY_GROUPS = [
    [(2 * b + j) * SIDE + 2 * a + i for j in range(2) for i in range(2)]
    for b in range(4)
    for a in range(4)
]
KEY_GROUPS = [
    [(2 * b + j) * SIDE + 2 * a + i for b in range(4) for a in range(4)]
    for j in range(2)
    for i in range(2)
]


def dot_nt(a, b):
    return lax.dot_general(a, b, (((1,), (1,)), ((), ())), preferred_element_type=jnp.float32)


def dot_tn(a, b):
    return lax.dot_general(a, b, (((0,), (0,)), ((), ())), preferred_element_type=jnp.float32)


def dot(a, b):
    return jnp.dot(a, b, preferred_element_type=jnp.float32)


def heads_down(q):
    return jnp.concatenate([q[:, h * HEAD : (h + 1) * HEAD] for h in range(HEADS)], axis=0)


def heads_across(o):
    return jnp.concatenate(
        [o[:, h * HEAD : (h + 1) * HEAD].T for h in range(HEADS)], axis=1
    )


def prep_kernel(q_ref, k_ref, v_ref, kv_out, q_out):
    kv = jnp.concatenate([k_ref[:LONG_DEV], v_ref[:LONG_DEV].T], axis=1)
    for i in range(kv_out.shape[0]):
        kv_out[i] = kv
    q = heads_across(q_ref[:LONG_DEV])
    for j in range(q_out.shape[0]):
        q_out[j] = q


def short_rows(q_ref, k_ref, v_ref, seg_ref):
    qs = heads_down(q_ref[LONG_DEV:])
    k = k_ref[LONG_DEV:]
    v = v_ref[LONG_DEV:]
    n = k.shape[0]
    seg_q = jnp.broadcast_to(seg_ref[...].astype(jnp.float32), (n, n))
    seg_k = seg_q.T
    row = lax.broadcasted_iota(jnp.int32, (n, n), 0)
    col = lax.broadcasted_iota(jnp.int32, (n, n), 1)
    visible = jnp.where((seg_q == seg_k) & (row <= col), 1.0, 0.0)
    visible = jnp.concatenate([visible] * HEADS, axis=1) > 0.5
    s = dot_nt(k, qs) * SCALE
    s = jnp.where(visible, s, FAR)
    top = jnp.max(s, axis=0, keepdims=True)
    w = jnp.where(visible, jnp.exp(s - top), 0.0)
    total = jnp.sum(w, axis=0, keepdims=True)
    o = dot_tn(v, w.astype(jnp.bfloat16)) / total
    return heads_across(o).astype(jnp.bfloat16)


def three_parts(x):
    high = x.astype(jnp.bfloat16).astype(jnp.float32)
    rest = x - high
    middle = rest.astype(jnp.bfloat16).astype(jnp.float32)
    return high, middle, rest - middle


def attend_kernel(
    wide_ref, span_ref, q_ref, kv_ref, out_ref, list_ref, top_ref, sum_ref, acc_ref
):
    j = pl.program_id(0)
    w = wide_ref[0]
    y = w // SIDE
    x = w % SIDE
    q_span = span_ref[((y // 2) * 2 + j // 2) * SIDE + (x // 2) * 2 + j % 2]
    qs = q_ref[j]
    cols = qs.shape[1]
    half = cols // 2
    count = jnp.int32(0)
    for i in range(kv_ref.shape[0]):
        span = span_ref[((i // 4) * 2 + y % 2) * SIDE + (i % 4) * 2 + x % 2]
        list_ref[count] = i
        count = count + jnp.where(span < q_span, 1, 0)
    for i in range(STEP):
        list_ref[count + i] = 0
    own = j == (y % 2) * 2 + x % 2

    @pl.when(own)
    def _():
        kv = kv_ref[(y // 2) * 4 + x // 2]
        row = lax.broadcasted_iota(jnp.int32, (LONG_DEV, cols), 0)
        col = lax.broadcasted_iota(jnp.int32, (LONG_DEV, cols), 1)
        s = jnp.where(row <= col % LONG_DEV, dot(kv[:, :HEAD], qs), FAR)
        top = jnp.max(s, axis=0, keepdims=True)
        p = jnp.exp2((s - top) * SCALE2)
        top_ref[...] = top
        sum_ref[...] = jnp.sum(p, axis=0, keepdims=True)
        acc_ref[...] = dot(kv[:, HEAD:], p.astype(jnp.bfloat16))

    @pl.when(jnp.logical_not(own))
    def _():
        top_ref[...] = jnp.full(top_ref.shape, FAR, jnp.float32)
        sum_ref[...] = jnp.zeros(sum_ref.shape, jnp.float32)
        acc_ref[...] = jnp.zeros(acc_ref.shape, jnp.float32)

    def advance(t, last):
        ids = [list_ref[t * STEP + u] for u in range(STEP)]
        k = jnp.concatenate([kv_ref[i, :, :HEAD] for i in ids], axis=0)
        v = jnp.concatenate([kv_ref[i, :, HEAD:] for i in ids], axis=1)
        scores = [dot(k, qs[:, g * half : (g + 1) * half]) for g in range(2)]
        for g, s in enumerate(scores):
            if last:
                s = jnp.concatenate(
                    [
                        jnp.where(t * STEP + u < count, s[u * LONG_DEV : (u + 1) * LONG_DEV], FAR)
                        for u in range(STEP)
                    ],
                    axis=0,
                )
            at = slice(g * half, (g + 1) * half)
            old = top_ref[:, at]
            new = jnp.maximum(old, jnp.max(s, axis=0, keepdims=True))
            p = jnp.exp2((s - new) * SCALE2)
            factor = jnp.exp2((old - new) * SCALE2)
            top_ref[:, at] = new
            sum_ref[:, at] = sum_ref[:, at] * factor + jnp.sum(p, axis=0, keepdims=True)
            acc_ref[:, at] = acc_ref[:, at] * factor + dot(v, p.astype(jnp.bfloat16))

    def step(t, carry):
        advance(t, False)
        return carry

    lax.fori_loop(0, count // STEP, step, 0)

    @pl.when(count % STEP > 0)
    def _():
        advance(count // STEP, True)

    total = sum_ref[...]
    o = acc_ref[...] / jnp.where(total > 0.0, total, 1.0)
    out_ref[0, :HEAD] = o.astype(jnp.bfloat16)
    parts = (*three_parts(top_ref[...] * SCALE2), *three_parts(total))
    row = lax.broadcasted_iota(jnp.int32, (STATS, cols), 0)
    stats = jnp.zeros((STATS, cols), jnp.float32)
    for i, part in enumerate(parts):
        stats = jnp.where(row == i, part, stats)
    out_ref[0, HEAD:] = stats.astype(jnp.bfloat16)


def merged_rows(got_ref):
    tops, sums = [], []
    for j in range(got_ref.shape[0]):
        stats = got_ref[j, HEAD:].astype(jnp.float32)
        tops.append(stats[0:1] + stats[1:2] + stats[2:3])
        sums.append(stats[3:4] + stats[4:5] + stats[5:6])
    top = jnp.maximum(jnp.maximum(tops[0], tops[1]), jnp.maximum(tops[2], tops[3]))
    shares = [s * jnp.exp2(t - top) for s, t in zip(sums, tops)]
    total = (shares[0] + shares[1]) + (shares[2] + shares[3])
    o = got_ref[0, :HEAD].astype(jnp.float32) * (shares[0] / total)
    for j in range(1, 4):
        o = o + got_ref[j, :HEAD].astype(jnp.float32) * (shares[j] / total)
    return heads_across(o).astype(jnp.bfloat16)


def projector(make_rows):
    def kernel(core_ref, *refs):
        *inputs, weight_ref, send_ref, keep_ref, rows_ref = refs
        half = rows_ref.shape[0] // 2

        @pl.when(pl.program_id(0) == 0)
        def _():
            made = make_rows(*inputs)
            core = core_ref[0]
            for b in range(2):
                at = pl.multiple_of(jnp.where(core == b, half, 0), half)
                rows_ref[pl.ds(at, half), :] = made[b * half : (b + 1) * half]

        product = dot(rows_ref[...], weight_ref[...])
        rounded = product.astype(jnp.bfloat16)
        send_ref[...] = rounded[:half]
        keep_ref[...] = rounded[half:]

    return kernel


def whole(x):
    return pl.BlockSpec(x.shape, lambda *i: (0,) * x.ndim)


def project(make_rows, core, inputs, specs, weight, name):
    cols, width = weight.shape
    half = LONG_DEV // 2
    block = 1024
    out = pl.BlockSpec((half, block), lambda i, c: (0, i))
    shape = jax.ShapeDtypeStruct((half, width), jnp.bfloat16)
    return pl.pallas_call(
        projector(make_rows),
        grid_spec=pltpu.PrefetchScalarGridSpec(
            num_scalar_prefetch=1,
            grid=(width // block,),
            in_specs=[
                *specs,
                pl.BlockSpec((cols, block), lambda i, c: (0, i)),
            ],
            out_specs=[out, out],
            scratch_shapes=[pltpu.VMEM((2 * half, cols), jnp.bfloat16)],
        ),
        out_shape=(shape, shape),
        name=name,
    )(core, *inputs, weight)


def pair_sum(a, b):
    return (a.astype(jnp.float32) + b.astype(jnp.float32)).astype(jnp.bfloat16)


def route_kernel(base_ref, far_ref, gain_ref, owner_ref, hidden_ref, out_ref, wide_ref):
    hidden = (base_ref[...] + far_ref[...].astype(jnp.float32)).astype(jnp.bfloat16)
    hidden_ref[...] = hidden
    h = hidden.astype(jnp.float32)
    mean = jnp.mean(h * h, axis=1, keepdims=True)
    normed = (h * lax.rsqrt(mean + 1e-05) * gain_ref[...].astype(jnp.float32)).astype(jnp.bfloat16)
    rows = h.shape[0]
    down = jnp.broadcast_to(owner_ref[...].astype(jnp.float32), (rows, HEAD))
    across = down.T[:rows]
    row = lax.broadcasted_iota(jnp.int32, (rows, rows), 0)
    col = lax.broadcasted_iota(jnp.int32, (rows, rows), 1)
    same = (down[:, :rows] == across) & (row < col)
    slot = jnp.sum(jnp.where(same, 1.0, 0.0), axis=0, keepdims=True)
    mine = across == row.astype(jnp.float32)
    owners = rows
    stride = out_ref.shape[0] // owners
    for s in range(2):
        pick = jnp.where(mine & (slot == float(s)), 1.0, 0.0).astype(jnp.bfloat16)
        placed = jnp.dot(pick, normed, preferred_element_type=jnp.float32)
        for t in range(stride // 2):
            wide_ref[pl.ds(s * (stride // 2) + t, owners, stride=stride), :] = placed[
                :, t * HEAD : (t + 1) * HEAD
            ]
    out_ref[...] = wide_ref[...].astype(jnp.bfloat16)


def in_vmem(x):
    return pltpu.with_memory_space_constraint(x, pltpu.VMEM)


def exchange(x, groups=None):
    return lax.all_to_all(x, "wide", 0, 0, tiled=True, axis_index_groups=groups)


def on_device(
    queries, key_rows, value_rows, residual, out_weight, norm_gain, span_map, segments, row_owner
):
    wide = lax.axis_index("wide").astype(jnp.int32).reshape(1)
    narrow = lax.axis_index("narrow").astype(jnp.int32).reshape(1)
    core = narrow & 1
    level = lax.shift_right_logical(narrow, jnp.ones_like(narrow))
    bf = jnp.bfloat16
    cols = queries.shape[1]
    width = out_weight.shape[1]
    vmem = pl.BlockSpec(memory_space=pltpu.VMEM)
    kv, qs = pl.pallas_call(
        prep_kernel,
        grid=(1,),
        in_specs=[whole(x) for x in (queries, key_rows, value_rows)],
        out_specs=(
            pl.BlockSpec((16, LONG_DEV, 2 * HEAD), lambda i: (0, 0, 0)),
            pl.BlockSpec((4, LONG_DEV, cols), lambda i: (0, 0, 0)),
        ),
        out_shape=(
            jax.ShapeDtypeStruct((16, LONG_DEV, 2 * HEAD), bf),
            jax.ShapeDtypeStruct((4, LONG_DEV, cols), bf),
        ),
        name="prep",
    )(queries, key_rows, value_rows)
    across = [(0, 1), (1, 0), (2, 3), (3, 2)]
    kv, qs, core_after = lax.optimization_barrier((kv, qs, core))
    kv = exchange(kv, KEY_GROUPS)
    qs = exchange(qs, QUERY_GROUPS)
    short_in = (queries, key_rows, value_rows, segments)
    send, keep_short = project(
        short_rows, core_after, short_in, [whole(x) for x in short_in], out_weight, "short"
    )
    near_short = lax.ppermute(send, "narrow", across)
    pair_short = pair_sum(keep_short, near_short)
    far_short = lax.ppermute(pair_short, "narrow", [(0, 2), (1, 3)])
    short = (keep_short.astype(jnp.float32) + near_short.astype(jnp.float32)) + far_short.astype(
        jnp.float32
    )
    wide, short = lax.optimization_barrier((wide, short))
    parts = pl.pallas_call(
        attend_kernel,
        grid_spec=pltpu.PrefetchScalarGridSpec(
            num_scalar_prefetch=2,
            grid=(4,),
            in_specs=[vmem, vmem],
            out_specs=pl.BlockSpec((1, HEAD + STATS, cols), lambda j, w, m: (j, 0, 0)),
            scratch_shapes=[
                pltpu.SMEM((16 + STEP,), jnp.int32),
                pltpu.VMEM((1, cols), jnp.float32),
                pltpu.VMEM((1, cols), jnp.float32),
                pltpu.VMEM((HEAD, cols), jnp.float32),
            ],
        ),
        out_shape=jax.ShapeDtypeStruct((4, HEAD + STATS, cols), bf),
        name="attend",
        compiler_params=ROOM,
    )(wide, span_map, in_vmem(qs), in_vmem(kv))
    got = exchange(parts, QUERY_GROUPS)
    send, keep = project(merged_rows, core, (in_vmem(got),), [vmem], out_weight, "long")
    near = lax.ppermute(send, "narrow", across)
    pair, keep, near = lax.optimization_barrier((pair_sum(keep, near), keep, near))
    far = lax.ppermute(pair, "narrow", [(2, 0), (3, 1)])
    long = keep.astype(jnp.float32) + near.astype(jnp.float32)
    base = residual.astype(jnp.float32) + jnp.where(level[0] == 0, long, short)
    rows = residual.shape[0]
    owners = 64
    tiles = 2 * width // HEAD
    hidden, outgoing = pl.pallas_call(
        route_kernel,
        in_specs=[vmem] * 4,
        out_shape=(
            jax.ShapeDtypeStruct((rows, width), bf),
            jax.ShapeDtypeStruct((owners * tiles, HEAD), bf),
        ),
        scratch_shapes=[pltpu.VMEM((owners * tiles, HEAD), jnp.float32)],
        name="route",
        compiler_params=ROOM,
    )(in_vmem(base), in_vmem(far), norm_gain.reshape(1, width), row_owner)
    arrived = exchange(outgoing.reshape(owners, tiles, HEAD))
    return (hidden, arrived.reshape(1, 1, owners, 2, width))


def solution(mesh):
    placed = (
        P(("rep", "wide"), "narrow"),
        P(("rep", "wide"), "narrow"),
        P(("rep", "wide"), "narrow"),
        P(("rep", "wide", "narrow"), None),
        P("narrow", None),
        P(),
        P(),
        P(("rep", "wide"), None),
        P(("rep", "wide", "narrow"), None),
    )
    return jax.shard_map(
        on_device,
        mesh=mesh,
        in_specs=placed,
        out_specs=(
            P(("rep", "wide", "narrow"), None),
            P(("rep", "wide"), "narrow", None, None, None),
        ),
        check_vma=False,
    )
```

```python
import jax
import jax.numpy as jnp
from jax import lax
from jax.experimental import pallas as pl
from jax.experimental.pallas import tpu as pltpu
from jax.sharding import PartitionSpec as P

HEAD = 128
LONG_DEV = 128
SIDE = 8
HEADS = 4
SCALE = HEAD ** (-0.5)
FAR = -1e30
ROOM = pltpu.CompilerParams(vmem_limit_bytes=24 * 1024 * 1024)
STATS = 16
FLIPS = (1, SIDE, SIDE + 1)
STEP = 4
SCALE2 = SCALE * 1.4426950408889634
QUERY_GROUPS = [
    [(2 * b + j) * SIDE + 2 * a + i for j in range(2) for i in range(2)]
    for b in range(4)
    for a in range(4)
]
KEY_GROUPS = [
    [(2 * b + j) * SIDE + 2 * a + i for b in range(4) for a in range(4)]
    for j in range(2)
    for i in range(2)
]


def dot_nt(a, b):
    return lax.dot_general(a, b, (((1,), (1,)), ((), ())), preferred_element_type=jnp.float32)


def dot_tn(a, b):
    return lax.dot_general(a, b, (((0,), (0,)), ((), ())), preferred_element_type=jnp.float32)


def dot(a, b):
    return jnp.dot(a, b, preferred_element_type=jnp.float32)


def heads_down(q):
    return jnp.concatenate([q[:, h * HEAD : (h + 1) * HEAD] for h in range(HEADS)], axis=0)


def heads_across(o):
    return jnp.concatenate(
        [o[:, h * HEAD : (h + 1) * HEAD].T for h in range(HEADS)], axis=1
    )


def prep_kernel(q_ref, k_ref, v_ref, kv_out, q_out):
    kv = jnp.concatenate([k_ref[:LONG_DEV], v_ref[:LONG_DEV].T], axis=1)
    for i in range(kv_out.shape[0]):
        kv_out[i] = kv
    q_out[...] = heads_across(q_ref[:LONG_DEV])


def short_rows(q_ref, k_ref, v_ref, seg_ref):
    qs = heads_down(q_ref[LONG_DEV:])
    k = k_ref[LONG_DEV:]
    v = v_ref[LONG_DEV:]
    n = k.shape[0]
    seg_q = jnp.broadcast_to(seg_ref[...].astype(jnp.float32), (n, n))
    seg_k = seg_q.T
    row = lax.broadcasted_iota(jnp.int32, (n, n), 0)
    col = lax.broadcasted_iota(jnp.int32, (n, n), 1)
    visible = jnp.where((seg_q == seg_k) & (row <= col), 1.0, 0.0)
    visible = jnp.concatenate([visible] * HEADS, axis=1) > 0.5
    s = dot_nt(k, qs) * SCALE
    s = jnp.where(visible, s, FAR)
    top = jnp.max(s, axis=0, keepdims=True)
    w = jnp.where(visible, jnp.exp(s - top), 0.0)
    total = jnp.sum(w, axis=0, keepdims=True)
    o = dot_tn(v, w.astype(jnp.bfloat16)) / total
    return heads_across(o).astype(jnp.bfloat16)


def three_parts(x):
    high = x.astype(jnp.bfloat16).astype(jnp.float32)
    rest = x - high
    middle = rest.astype(jnp.bfloat16).astype(jnp.float32)
    return high, middle, rest - middle


def member(w):
    return (w // SIDE % 2) * 2 + w % 2


def attend_kernel(
    wide_ref,
    span_ref,
    q0_ref,
    q1_ref,
    q2_ref,
    q3_ref,
    kv_ref,
    out_ref,
    list_ref,
    q_ref,
    top_ref,
    sum_ref,
    acc_ref,
):
    r = pl.program_id(0)
    w = wide_ref[0]
    y = w // SIDE
    x = w % SIDE
    j = r ^ member(w)

    @pl.when(r == 0)
    def _():
        for i, ref in enumerate((q0_ref, q1_ref, q2_ref, q3_ref)):
            q_ref[i] = ref[...]

    q_span = span_ref[((y // 2) * 2 + j // 2) * SIDE + (x // 2) * 2 + j % 2]
    qs = q_ref[r]
    cols = qs.shape[1]
    half = cols // 2
    count = jnp.int32(0)
    for i in range(kv_ref.shape[0]):
        span = span_ref[((i // 4) * 2 + y % 2) * SIDE + (i % 4) * 2 + x % 2]
        list_ref[count] = i
        count = count + jnp.where(span < q_span, 1, 0)
    for i in range(STEP):
        list_ref[count + i] = 0
    own = r == 0

    @pl.when(own)
    def _():
        kv = kv_ref[(y // 2) * 4 + x // 2]
        row = lax.broadcasted_iota(jnp.int32, (LONG_DEV, cols), 0)
        col = lax.broadcasted_iota(jnp.int32, (LONG_DEV, cols), 1)
        s = jnp.where(row <= col % LONG_DEV, dot(kv[:, :HEAD], qs), FAR)
        top = jnp.max(s, axis=0, keepdims=True)
        p = jnp.exp2((s - top) * SCALE2)
        top_ref[...] = top
        sum_ref[...] = jnp.sum(p, axis=0, keepdims=True)
        acc_ref[...] = dot(kv[:, HEAD:], p.astype(jnp.bfloat16))

    @pl.when(jnp.logical_not(own))
    def _():
        top_ref[...] = jnp.full(top_ref.shape, FAR, jnp.float32)
        sum_ref[...] = jnp.zeros(sum_ref.shape, jnp.float32)
        acc_ref[...] = jnp.zeros(acc_ref.shape, jnp.float32)

    def advance(t, last):
        ids = [list_ref[t * STEP + u] for u in range(STEP)]
        k = jnp.concatenate([kv_ref[i, :, :HEAD] for i in ids], axis=0)
        v = jnp.concatenate([kv_ref[i, :, HEAD:] for i in ids], axis=1)
        scores = [dot(k, qs[:, g * half : (g + 1) * half]) for g in range(2)]
        for g, s in enumerate(scores):
            if last:
                s = jnp.concatenate(
                    [
                        jnp.where(t * STEP + u < count, s[u * LONG_DEV : (u + 1) * LONG_DEV], FAR)
                        for u in range(STEP)
                    ],
                    axis=0,
                )
            at = slice(g * half, (g + 1) * half)
            old = top_ref[:, at]
            new = jnp.maximum(old, jnp.max(s, axis=0, keepdims=True))
            p = jnp.exp2((s - new) * SCALE2)
            factor = jnp.exp2((old - new) * SCALE2)
            top_ref[:, at] = new
            sum_ref[:, at] = sum_ref[:, at] * factor + jnp.sum(p, axis=0, keepdims=True)
            acc_ref[:, at] = acc_ref[:, at] * factor + dot(v, p.astype(jnp.bfloat16))

    def step(t, carry):
        advance(t, False)
        return carry

    lax.fori_loop(0, count // STEP, step, 0)

    @pl.when(count % STEP > 0)
    def _():
        advance(count // STEP, True)

    total = sum_ref[...]
    o = acc_ref[...] / jnp.where(total > 0.0, total, 1.0)
    out_ref[0, :HEAD] = o.astype(jnp.bfloat16)
    parts = (*three_parts(top_ref[...] * SCALE2), *three_parts(total))
    row = lax.broadcasted_iota(jnp.int32, (STATS, cols), 0)
    stats = jnp.zeros((STATS, cols), jnp.float32)
    for i, part in enumerate(parts):
        stats = jnp.where(row == i, part, stats)
    out_ref[0, HEAD:] = stats.astype(jnp.bfloat16)


def merged_rows(got_ref):
    tops, sums = [], []
    for j in range(got_ref.shape[0]):
        stats = got_ref[j, HEAD:].astype(jnp.float32)
        tops.append(stats[0:1] + stats[1:2] + stats[2:3])
        sums.append(stats[3:4] + stats[4:5] + stats[5:6])
    top = jnp.maximum(jnp.maximum(tops[0], tops[1]), jnp.maximum(tops[2], tops[3]))
    shares = [s * jnp.exp2(t - top) for s, t in zip(sums, tops)]
    total = (shares[0] + shares[1]) + (shares[2] + shares[3])
    o = got_ref[0, :HEAD].astype(jnp.float32) * (shares[0] / total)
    for j in range(1, 4):
        o = o + got_ref[j, :HEAD].astype(jnp.float32) * (shares[j] / total)
    return heads_across(o).astype(jnp.bfloat16)


def projector(make_rows):
    def kernel(core_ref, *refs):
        *inputs, weight_ref, send_ref, keep_ref, rows_ref = refs
        half = rows_ref.shape[0] // 2

        @pl.when(pl.program_id(0) == 0)
        def _():
            made = make_rows(*inputs)
            core = core_ref[0]
            for b in range(2):
                at = pl.multiple_of(jnp.where(core == b, half, 0), half)
                rows_ref[pl.ds(at, half), :] = made[b * half : (b + 1) * half]

        product = dot(rows_ref[...], weight_ref[...])
        rounded = product.astype(jnp.bfloat16)
        send_ref[...] = rounded[:half]
        keep_ref[...] = rounded[half:]

    return kernel


def whole(x):
    return pl.BlockSpec(x.shape, lambda *i: (0,) * x.ndim)


def project(make_rows, core, inputs, specs, weight):
    cols, width = weight.shape
    half = LONG_DEV // 2
    block = 1024
    out = pl.BlockSpec((half, block), lambda i, c: (0, i))
    shape = jax.ShapeDtypeStruct((half, width), jnp.bfloat16)
    return pl.pallas_call(
        projector(make_rows),
        grid_spec=pltpu.PrefetchScalarGridSpec(
            num_scalar_prefetch=1,
            grid=(width // block,),
            in_specs=[
                *specs,
                pl.BlockSpec((cols, block), lambda i, c: (0, i)),
            ],
            out_specs=[out, out],
            scratch_shapes=[pltpu.VMEM((2 * half, cols), jnp.bfloat16)],
        ),
        out_shape=(shape, shape),
    )(core, *inputs, weight)


def pair_sum(a, b):
    return (a.astype(jnp.float32) + b.astype(jnp.float32)).astype(jnp.bfloat16)


def route_kernel(base_ref, far_ref, gain_ref, owner_ref, hidden_ref, out_ref, wide_ref):
    hidden = (base_ref[...] + far_ref[...].astype(jnp.float32)).astype(jnp.bfloat16)
    hidden_ref[...] = hidden
    h = hidden.astype(jnp.float32)
    mean = jnp.mean(h * h, axis=1, keepdims=True)
    normed = (h * lax.rsqrt(mean + 1e-05) * gain_ref[...].astype(jnp.float32)).astype(jnp.bfloat16)
    rows = h.shape[0]
    down = jnp.broadcast_to(owner_ref[...].astype(jnp.float32), (rows, HEAD))
    across = down.T[:rows]
    row = lax.broadcasted_iota(jnp.int32, (rows, rows), 0)
    col = lax.broadcasted_iota(jnp.int32, (rows, rows), 1)
    same = (down[:, :rows] == across) & (row < col)
    slot = jnp.sum(jnp.where(same, 1.0, 0.0), axis=0, keepdims=True)
    mine = across == row.astype(jnp.float32)
    owners = rows
    stride = out_ref.shape[0] // owners
    for s in range(2):
        pick = jnp.where(mine & (slot == float(s)), 1.0, 0.0).astype(jnp.bfloat16)
        placed = jnp.dot(pick, normed, preferred_element_type=jnp.float32)
        for t in range(stride // 2):
            wide_ref[pl.ds(s * (stride // 2) + t, owners, stride=stride), :] = placed[
                :, t * HEAD : (t + 1) * HEAD
            ]
    out_ref[...] = wide_ref[...].astype(jnp.bfloat16)


def in_vmem(x):
    return pltpu.with_memory_space_constraint(x, pltpu.VMEM)


def exchange(x, groups=None):
    return lax.all_to_all(x, "wide", 0, 0, tiled=True, axis_index_groups=groups)


def on_device(
    queries, key_rows, value_rows, residual, out_weight, norm_gain, span_map, segments, row_owner
):
    wide = lax.axis_index("wide").astype(jnp.int32).reshape(1)
    narrow = lax.axis_index("narrow").astype(jnp.int32).reshape(1)
    core = narrow & 1
    level = lax.shift_right_logical(narrow, jnp.ones_like(narrow))
    bf = jnp.bfloat16
    cols = queries.shape[1]
    width = out_weight.shape[1]
    vmem = pl.BlockSpec(memory_space=pltpu.VMEM)
    kv, qs = pl.pallas_call(
        prep_kernel,
        grid=(1,),
        in_specs=[whole(x) for x in (queries, key_rows, value_rows)],
        out_specs=(
            pl.BlockSpec((16, LONG_DEV, 2 * HEAD), lambda i: (0, 0, 0)),
            pl.BlockSpec((LONG_DEV, cols), lambda i: (0, 0)),
        ),
        out_shape=(
            jax.ShapeDtypeStruct((16, LONG_DEV, 2 * HEAD), bf),
            jax.ShapeDtypeStruct((LONG_DEV, cols), bf),
        ),
        name="prep",
    )(queries, key_rows, value_rows)
    across = [(0, 1), (1, 0), (2, 3), (3, 2)]
    kv, qs, core_after = lax.optimization_barrier((kv, qs, core))
    kv = exchange(kv, KEY_GROUPS)
    devices = range(SIDE * SIDE)
    queries_by = [qs] + [
        lax.ppermute(qs, "wide", [(i, i ^ flip) for i in devices]) for flip in FLIPS
    ]
    short_in = (queries, key_rows, value_rows, segments)
    send, keep_short = project(
        short_rows, core_after, short_in, [whole(x) for x in short_in], out_weight
    )
    near_short = lax.ppermute(send, "narrow", across)
    pair_short = pair_sum(keep_short, near_short)
    far_short = lax.ppermute(pair_short, "narrow", [(0, 2), (1, 3)])
    short = (keep_short.astype(jnp.float32) + near_short.astype(jnp.float32)) + far_short.astype(
        jnp.float32
    )
    wide, short = lax.optimization_barrier((wide, short))
    parts = pl.pallas_call(
        attend_kernel,
        grid_spec=pltpu.PrefetchScalarGridSpec(
            num_scalar_prefetch=2,
            grid=(4,),
            in_specs=[vmem] * 5,
            out_specs=pl.BlockSpec(
                (1, HEAD + STATS, cols), lambda r, w, m: (r ^ member(w[0]), 0, 0)
            ),
            scratch_shapes=[
                pltpu.SMEM((16 + STEP,), jnp.int32),
                pltpu.VMEM((4, LONG_DEV, cols), bf),
                pltpu.VMEM((1, cols), jnp.float32),
                pltpu.VMEM((1, cols), jnp.float32),
                pltpu.VMEM((HEAD, cols), jnp.float32),
            ],
        ),
        out_shape=jax.ShapeDtypeStruct((4, HEAD + STATS, cols), bf),
        name="attend",
        compiler_params=ROOM,
    )(wide, span_map, *map(in_vmem, queries_by), in_vmem(kv))
    got = exchange(parts, QUERY_GROUPS)
    send, keep = project(merged_rows, core, (in_vmem(got),), [vmem], out_weight)
    near = lax.ppermute(send, "narrow", across)
    pair, keep, near = lax.optimization_barrier((pair_sum(keep, near), keep, near))
    far = lax.ppermute(pair, "narrow", [(2, 0), (3, 1)])
    long = keep.astype(jnp.float32) + near.astype(jnp.float32)
    base = residual.astype(jnp.float32) + jnp.where(level[0] == 0, long, short)
    rows = residual.shape[0]
    owners = 64
    tiles = 2 * width // HEAD
    hidden, outgoing = pl.pallas_call(
        route_kernel,
        in_specs=[vmem] * 4,
        out_shape=(
            jax.ShapeDtypeStruct((rows, width), bf),
            jax.ShapeDtypeStruct((owners * tiles, HEAD), bf),
        ),
        scratch_shapes=[pltpu.VMEM((owners * tiles, HEAD), jnp.float32)],
        name="route",
        compiler_params=ROOM,
    )(in_vmem(base), in_vmem(far), norm_gain.reshape(1, width), row_owner)
    arrived = exchange(outgoing.reshape(owners, tiles, HEAD))
    return (hidden, arrived.reshape(1, 1, owners, 2, width))


def solution(mesh):
    placed = (
        P(("rep", "wide"), "narrow"),
        P(("rep", "wide"), "narrow"),
        P(("rep", "wide"), "narrow"),
        P(("rep", "wide", "narrow"), None),
        P("narrow", None),
        P(),
        P(),
        P(("rep", "wide"), None),
        P(("rep", "wide", "narrow"), None),
    )
    return jax.shard_map(
        on_device,
        mesh=mesh,
        in_specs=placed,
        out_specs=(
            P(("rep", "wide", "narrow"), None),
            P(("rep", "wide"), "narrow", None, None, None),
        ),
        check_vma=False,
    )
```

```python
import jax
import jax.numpy as jnp
from jax import lax
from jax.experimental import pallas as pl
from jax.experimental.pallas import tpu as pltpu
from jax.sharding import PartitionSpec as P

HEAD = 128
LONG_DEV = 128
SIDE = 8
HEADS = 4
SCALE = HEAD ** (-0.5)
FAR = -1e30
ROOM = pltpu.CompilerParams(vmem_limit_bytes=24 * 1024 * 1024)
STATS = 16
FLIPS = (1, SIDE, SIDE + 1)
STEP = 4
SCALE2 = SCALE * 1.4426950408889634
QUERY_GROUPS = [
    [(2 * b + j) * SIDE + 2 * a + i for j in range(2) for i in range(2)]
    for b in range(4)
    for a in range(4)
]
KEY_GROUPS = [
    [(2 * b + j) * SIDE + 2 * a + i for b in range(4) for a in range(4)]
    for j in range(2)
    for i in range(2)
]


def dot_nt(a, b):
    return lax.dot_general(a, b, (((1,), (1,)), ((), ())), preferred_element_type=jnp.float32)


def dot_tn(a, b):
    return lax.dot_general(a, b, (((0,), (0,)), ((), ())), preferred_element_type=jnp.float32)


def dot(a, b):
    return jnp.dot(a, b, preferred_element_type=jnp.float32)


def heads_down(q):
    return jnp.concatenate([q[:, h * HEAD : (h + 1) * HEAD] for h in range(HEADS)], axis=0)


def heads_across(o):
    return jnp.concatenate(
        [o[:, h * HEAD : (h + 1) * HEAD].T for h in range(HEADS)], axis=1
    )


def prep_kernel(q_ref, k_ref, v_ref, kv_out, q_out):
    kv = jnp.concatenate([k_ref[:LONG_DEV], v_ref[:LONG_DEV].T], axis=1)
    for i in range(kv_out.shape[0]):
        kv_out[i] = kv
    q_out[...] = heads_across(q_ref[:LONG_DEV])


def short_rows(q_ref, k_ref, v_ref, seg_ref):
    qs = heads_down(q_ref[LONG_DEV:])
    k = k_ref[LONG_DEV:]
    v = v_ref[LONG_DEV:]
    n = k.shape[0]
    seg_q = jnp.broadcast_to(seg_ref[...].astype(jnp.float32), (n, n))
    seg_k = seg_q.T
    row = lax.broadcasted_iota(jnp.int32, (n, n), 0)
    col = lax.broadcasted_iota(jnp.int32, (n, n), 1)
    visible = jnp.where((seg_q == seg_k) & (row <= col), 1.0, 0.0)
    visible = jnp.concatenate([visible] * HEADS, axis=1) > 0.5
    s = dot_nt(k, qs) * SCALE
    s = jnp.where(visible, s, FAR)
    top = jnp.max(s, axis=0, keepdims=True)
    w = jnp.where(visible, jnp.exp(s - top), 0.0)
    total = jnp.sum(w, axis=0, keepdims=True)
    o = dot_tn(v, w.astype(jnp.bfloat16)) / total
    return heads_across(o).astype(jnp.bfloat16)


def three_parts(x):
    high = x.astype(jnp.bfloat16).astype(jnp.float32)
    rest = x - high
    middle = rest.astype(jnp.bfloat16).astype(jnp.float32)
    return high, middle, rest - middle


def member(w):
    return (w // SIDE % 2) * 2 + w % 2


def attend_kernel(
    wide_ref,
    span_ref,
    q0_ref,
    q1_ref,
    q2_ref,
    q3_ref,
    kv_ref,
    out_ref,
    list_ref,
    q_ref,
    top_ref,
    sum_ref,
    acc_ref,
):
    r = pl.program_id(0)
    w = wide_ref[0]
    y = w // SIDE
    x = w % SIDE
    j = r ^ member(w)

    @pl.when(r == 0)
    def _():
        for i, ref in enumerate((q0_ref, q1_ref, q2_ref, q3_ref)):
            q_ref[i] = ref[...]

    q_span = span_ref[((y // 2) * 2 + j // 2) * SIDE + (x // 2) * 2 + j % 2]
    qs = q_ref[r]
    cols = qs.shape[1]
    half = cols // 2
    count = jnp.int32(0)
    for i in range(kv_ref.shape[0]):
        span = span_ref[((i // 4) * 2 + y % 2) * SIDE + (i % 4) * 2 + x % 2]
        list_ref[count] = i
        count = count + jnp.where(span < q_span, 1, 0)
    for i in range(STEP):
        list_ref[count + i] = 0
    own = r == 0

    @pl.when(own)
    def _():
        kv = kv_ref[(y // 2) * 4 + x // 2]
        row = lax.broadcasted_iota(jnp.int32, (LONG_DEV, cols), 0)
        col = lax.broadcasted_iota(jnp.int32, (LONG_DEV, cols), 1)
        s = jnp.where(row <= col % LONG_DEV, dot(kv[:, :HEAD], qs), FAR)
        top = jnp.max(s, axis=0, keepdims=True)
        p = jnp.exp2((s - top) * SCALE2)
        top_ref[...] = top
        sum_ref[...] = jnp.sum(p, axis=0, keepdims=True)
        acc_ref[...] = dot(kv[:, HEAD:], p.astype(jnp.bfloat16))

    @pl.when(jnp.logical_not(own))
    def _():
        top_ref[...] = jnp.full(top_ref.shape, FAR, jnp.float32)
        sum_ref[...] = jnp.zeros(sum_ref.shape, jnp.float32)
        acc_ref[...] = jnp.zeros(acc_ref.shape, jnp.float32)

    def advance(t, last):
        ids = [list_ref[t * STEP + u] for u in range(STEP)]
        k = jnp.concatenate([kv_ref[i, :, :HEAD] for i in ids], axis=0)
        v = jnp.concatenate([kv_ref[i, :, HEAD:] for i in ids], axis=1)
        scores = [dot(k, qs[:, g * half : (g + 1) * half]) for g in range(2)]
        for g, s in enumerate(scores):
            if last:
                s = jnp.concatenate(
                    [
                        jnp.where(t * STEP + u < count, s[u * LONG_DEV : (u + 1) * LONG_DEV], FAR)
                        for u in range(STEP)
                    ],
                    axis=0,
                )
            at = slice(g * half, (g + 1) * half)
            old = top_ref[:, at]
            new = jnp.maximum(old, jnp.max(s, axis=0, keepdims=True))
            p = jnp.exp2((s - new) * SCALE2)
            factor = jnp.exp2((old - new) * SCALE2)
            top_ref[:, at] = new
            sum_ref[:, at] = sum_ref[:, at] * factor + jnp.sum(p, axis=0, keepdims=True)
            acc_ref[:, at] = acc_ref[:, at] * factor + dot(v, p.astype(jnp.bfloat16))

    def step(t, carry):
        advance(t, False)
        return carry

    lax.fori_loop(0, count // STEP, step, 0)

    @pl.when(count % STEP > 0)
    def _():
        advance(count // STEP, True)

    total = sum_ref[...]
    o = acc_ref[...] / jnp.where(total > 0.0, total, 1.0)
    out_ref[0, :HEAD] = o.astype(jnp.bfloat16)
    parts = (*three_parts(top_ref[...] * SCALE2), *three_parts(total))
    row = lax.broadcasted_iota(jnp.int32, (STATS, cols), 0)
    stats = jnp.zeros((STATS, cols), jnp.float32)
    for i, part in enumerate(parts):
        stats = jnp.where(row == i, part, stats)
    out_ref[0, HEAD:] = stats.astype(jnp.bfloat16)


def merged_rows(got_ref):
    tops, sums = [], []
    for j in range(got_ref.shape[0]):
        stats = got_ref[j, HEAD:].astype(jnp.float32)
        tops.append(stats[0:1] + stats[1:2] + stats[2:3])
        sums.append(stats[3:4] + stats[4:5] + stats[5:6])
    top = jnp.maximum(jnp.maximum(tops[0], tops[1]), jnp.maximum(tops[2], tops[3]))
    shares = [s * jnp.exp2(t - top) for s, t in zip(sums, tops)]
    total = (shares[0] + shares[1]) + (shares[2] + shares[3])
    o = got_ref[0, :HEAD].astype(jnp.float32) * (shares[0] / total)
    for j in range(1, 4):
        o = o + got_ref[j, :HEAD].astype(jnp.float32) * (shares[j] / total)
    return heads_across(o).astype(jnp.bfloat16)


def projector(make_rows):
    def kernel(core_ref, *refs):
        *inputs, weight_ref, send_ref, keep_ref, rows_ref = refs
        half = rows_ref.shape[0] // 2

        @pl.when(pl.program_id(0) == 0)
        def _():
            made = make_rows(*inputs)
            core = core_ref[0]
            for b in range(2):
                at = pl.multiple_of(jnp.where(core == b, half, 0), half)
                rows_ref[pl.ds(at, half), :] = made[b * half : (b + 1) * half]

        product = dot(rows_ref[...], weight_ref[...])
        rounded = product.astype(jnp.bfloat16)
        send_ref[...] = rounded[:half]
        keep_ref[...] = rounded[half:]

    return kernel


def whole(x):
    return pl.BlockSpec(x.shape, lambda *i: (0,) * x.ndim)


def project(make_rows, core, inputs, specs, weight, parts=1):
    cols, width = weight.shape
    width = width // parts
    half = LONG_DEV // 2
    block = 1024
    out = pl.BlockSpec((half, block), lambda i, c: (0, i))
    shape = jax.ShapeDtypeStruct((half, width), jnp.bfloat16)
    return pl.pallas_call(
        projector(make_rows),
        grid_spec=pltpu.PrefetchScalarGridSpec(
            num_scalar_prefetch=1,
            grid=(width // block,),
            in_specs=[
                *specs,
                pl.BlockSpec((cols, block), lambda i, c: (0, i)),
            ],
            out_specs=[out, out, pl.BlockSpec((2 * half, cols), lambda i, c: (0, 0))],
        ),
        out_shape=(shape, shape, jax.ShapeDtypeStruct((2 * half, cols), jnp.bfloat16)),
    )(core, *inputs, weight)


def rest_kernel(rows_ref, weight_ref, send_ref, keep_ref):
    rounded = dot(rows_ref[...], weight_ref[...]).astype(jnp.bfloat16)
    half = send_ref.shape[0]
    send_ref[...] = rounded[:half]
    keep_ref[...] = rounded[half:]


def project_rest(rows, weight):
    cols, width = weight.shape
    width = width // 2
    half = LONG_DEV // 2
    block = 1024
    first = width // block
    out = pl.BlockSpec((half, block), lambda i: (0, i))
    shape = jax.ShapeDtypeStruct((half, width), jnp.bfloat16)
    return pl.pallas_call(
        rest_kernel,
        grid=(width // block,),
        in_specs=[
            pl.BlockSpec((2 * half, cols), lambda i: (0, 0)),
            pl.BlockSpec((cols, block), lambda i: (0, i + first)),
        ],
        out_specs=[out, out],
        out_shape=(shape, shape),
        name="rest",
    )(rows, weight)


def pair_sum(a, b):
    return (a.astype(jnp.float32) + b.astype(jnp.float32)).astype(jnp.bfloat16)


def route_kernel(
    base0_ref, base1_ref, far0_ref, far1_ref, gain_ref, owner_ref, hidden_ref, out_ref, wide_ref
):
    hidden = jnp.concatenate(
        [
            base_ref[...] + far_ref[...].astype(jnp.float32)
            for base_ref, far_ref in ((base0_ref, far0_ref), (base1_ref, far1_ref))
        ],
        axis=1,
    ).astype(jnp.bfloat16)
    hidden_ref[...] = hidden
    h = hidden.astype(jnp.float32)
    mean = jnp.mean(h * h, axis=1, keepdims=True)
    normed = (h * lax.rsqrt(mean + 1e-05) * gain_ref[...].astype(jnp.float32)).astype(jnp.bfloat16)
    rows = h.shape[0]
    down = jnp.broadcast_to(owner_ref[...].astype(jnp.float32), (rows, HEAD))
    across = down.T[:rows]
    row = lax.broadcasted_iota(jnp.int32, (rows, rows), 0)
    col = lax.broadcasted_iota(jnp.int32, (rows, rows), 1)
    same = (down[:, :rows] == across) & (row < col)
    slot = jnp.sum(jnp.where(same, 1.0, 0.0), axis=0, keepdims=True)
    mine = across == row.astype(jnp.float32)
    owners = rows
    stride = out_ref.shape[0] // owners
    for s in range(2):
        pick = jnp.where(mine & (slot == float(s)), 1.0, 0.0).astype(jnp.bfloat16)
        placed = jnp.dot(pick, normed, preferred_element_type=jnp.float32)
        for t in range(stride // 2):
            wide_ref[pl.ds(s * (stride // 2) + t, owners, stride=stride), :] = placed[
                :, t * HEAD : (t + 1) * HEAD
            ]
    out_ref[...] = wide_ref[...].astype(jnp.bfloat16)


def in_vmem(x):
    return pltpu.with_memory_space_constraint(x, pltpu.VMEM)


def exchange(x, groups=None):
    return lax.all_to_all(x, "wide", 0, 0, tiled=True, axis_index_groups=groups)


def on_device(
    queries, key_rows, value_rows, residual, out_weight, norm_gain, span_map, segments, row_owner
):
    wide = lax.axis_index("wide").astype(jnp.int32).reshape(1)
    narrow = lax.axis_index("narrow").astype(jnp.int32).reshape(1)
    core = narrow & 1
    level = lax.shift_right_logical(narrow, jnp.ones_like(narrow))
    bf = jnp.bfloat16
    cols = queries.shape[1]
    width = out_weight.shape[1]
    vmem = pl.BlockSpec(memory_space=pltpu.VMEM)
    kv, qs = pl.pallas_call(
        prep_kernel,
        grid=(1,),
        in_specs=[whole(x) for x in (queries, key_rows, value_rows)],
        out_specs=(
            pl.BlockSpec((16, LONG_DEV, 2 * HEAD), lambda i: (0, 0, 0)),
            pl.BlockSpec((LONG_DEV, cols), lambda i: (0, 0)),
        ),
        out_shape=(
            jax.ShapeDtypeStruct((16, LONG_DEV, 2 * HEAD), bf),
            jax.ShapeDtypeStruct((LONG_DEV, cols), bf),
        ),
        name="prep",
    )(queries, key_rows, value_rows)
    across = [(0, 1), (1, 0), (2, 3), (3, 2)]
    kv, qs, core_after = lax.optimization_barrier((kv, qs, core))
    kv = exchange(kv, KEY_GROUPS)
    devices = range(SIDE * SIDE)
    queries_by = [qs] + [
        lax.ppermute(qs, "wide", [(i, i ^ flip) for i in devices]) for flip in FLIPS
    ]
    short_in = (queries, key_rows, value_rows, segments)
    send, keep_short, _ = project(
        short_rows, core_after, short_in, [whole(x) for x in short_in], out_weight
    )
    near_short = lax.ppermute(send, "narrow", across)
    pair_short = pair_sum(keep_short, near_short)
    far_short = lax.ppermute(pair_short, "narrow", [(0, 2), (1, 3)])
    short = (keep_short.astype(jnp.float32) + near_short.astype(jnp.float32)) + far_short.astype(
        jnp.float32
    )
    wide, short = lax.optimization_barrier((wide, short))
    parts = pl.pallas_call(
        attend_kernel,
        grid_spec=pltpu.PrefetchScalarGridSpec(
            num_scalar_prefetch=2,
            grid=(4,),
            in_specs=[vmem] * 5,
            out_specs=pl.BlockSpec(
                (1, HEAD + STATS, cols), lambda r, w, m: (r ^ member(w[0]), 0, 0)
            ),
            scratch_shapes=[
                pltpu.SMEM((16 + STEP,), jnp.int32),
                pltpu.VMEM((4, LONG_DEV, cols), bf),
                pltpu.VMEM((1, cols), jnp.float32),
                pltpu.VMEM((1, cols), jnp.float32),
                pltpu.VMEM((HEAD, cols), jnp.float32),
            ],
        ),
        out_shape=jax.ShapeDtypeStruct((4, HEAD + STATS, cols), bf),
        name="attend",
        compiler_params=ROOM,
    )(wide, span_map, *map(in_vmem, queries_by), in_vmem(kv))
    got = exchange(parts, QUERY_GROUPS)
    send, keep, placed = project(merged_rows, core, (in_vmem(got),), [vmem], out_weight, parts=2)
    near = lax.ppermute(send, "narrow", across)
    send_rest, keep_rest = project_rest(placed, out_weight)
    near_rest = lax.ppermute(send_rest, "narrow", across)
    bases, fars = [], []
    for part, (k, n) in enumerate(((keep, near), (keep_rest, near_rest))):
        pair, k, n = lax.optimization_barrier((pair_sum(k, n), k, n))
        fars.append(lax.ppermute(pair, "narrow", [(2, 0), (3, 1)]))
        at = slice(part * width // 2, (part + 1) * width // 2)
        long = k.astype(jnp.float32) + n.astype(jnp.float32)
        bases.append(
            residual[:, at].astype(jnp.float32) + jnp.where(level[0] == 0, long, short[:, at])
        )
    rows = residual.shape[0]
    owners = 64
    tiles = 2 * width // HEAD
    hidden, outgoing = pl.pallas_call(
        route_kernel,
        in_specs=[vmem] * 6,
        out_shape=(
            jax.ShapeDtypeStruct((rows, width), bf),
            jax.ShapeDtypeStruct((owners * tiles, HEAD), bf),
        ),
        scratch_shapes=[pltpu.VMEM((owners * tiles, HEAD), jnp.float32)],
        name="route",
        compiler_params=ROOM,
    )(*map(in_vmem, bases), *map(in_vmem, fars), norm_gain.reshape(1, width), row_owner)
    arrived = exchange(outgoing.reshape(owners, tiles, HEAD))
    return (hidden, arrived.reshape(1, 1, owners, 2, width))


def solution(mesh):
    placed = (
        P(("rep", "wide"), "narrow"),
        P(("rep", "wide"), "narrow"),
        P(("rep", "wide"), "narrow"),
        P(("rep", "wide", "narrow"), None),
        P("narrow", None),
        P(),
        P(),
        P(("rep", "wide"), None),
        P(("rep", "wide", "narrow"), None),
    )
    return jax.shard_map(
        on_device,
        mesh=mesh,
        in_specs=placed,
        out_specs=(
            P(("rep", "wide", "narrow"), None),
            P(("rep", "wide"), "narrow", None, None, None),
        ),
        check_vma=False,
    )
```

```python
import jax
import jax.numpy as jnp
from jax import lax
from jax.experimental import pallas as pl
from jax.experimental.pallas import tpu as pltpu
from jax.sharding import PartitionSpec as P

HEAD = 128
LONG_DEV = 128
SIDE = 8
HEADS = 4
SCALE = HEAD ** (-0.5)
FAR = -1e30
ROOM = pltpu.CompilerParams(vmem_limit_bytes=24 * 1024 * 1024)
STATS = 16
FLIPS = (1, SIDE, SIDE + 1)
STEP = 4
SCALE2 = SCALE * 1.4426950408889634
QUERY_GROUPS = [
    [(2 * b + j) * SIDE + 2 * a + i for j in range(2) for i in range(2)]
    for b in range(4)
    for a in range(4)
]
KEY_GROUPS = [
    [(2 * b + j) * SIDE + 2 * a + i for b in range(4) for a in range(4)]
    for j in range(2)
    for i in range(2)
]


def dot_nt(a, b):
    return lax.dot_general(a, b, (((1,), (1,)), ((), ())), preferred_element_type=jnp.float32)


def dot_tn(a, b):
    return lax.dot_general(a, b, (((0,), (0,)), ((), ())), preferred_element_type=jnp.float32)


def dot(a, b):
    return jnp.dot(a, b, preferred_element_type=jnp.float32)


def heads_down(q):
    return jnp.concatenate([q[:, h * HEAD : (h + 1) * HEAD] for h in range(HEADS)], axis=0)


def heads_across(o):
    return jnp.concatenate(
        [o[:, h * HEAD : (h + 1) * HEAD].T for h in range(HEADS)], axis=1
    )


def prep_kernel(q_ref, k_ref, v_ref, kv_out, q_out):
    kv = jnp.concatenate([k_ref[...], v_ref[...].T], axis=1)
    for i in range(kv_out.shape[0]):
        kv_out[i] = kv
    q_out[...] = heads_across(q_ref[...])


def short_rows(q_ref, k_ref, v_ref, seg_ref):
    qs = heads_down(q_ref[LONG_DEV:])
    k = k_ref[LONG_DEV:]
    v = v_ref[LONG_DEV:]
    n = k.shape[0]
    seg_q = jnp.broadcast_to(seg_ref[...].astype(jnp.float32), (n, n))
    seg_k = seg_q.T
    row = lax.broadcasted_iota(jnp.int32, (n, n), 0)
    col = lax.broadcasted_iota(jnp.int32, (n, n), 1)
    visible = jnp.where((seg_q == seg_k) & (row <= col), 1.0, 0.0)
    visible = jnp.concatenate([visible] * HEADS, axis=1) > 0.5
    s = dot_nt(k, qs) * SCALE
    s = jnp.where(visible, s, FAR)
    top = jnp.max(s, axis=0, keepdims=True)
    w = jnp.where(visible, jnp.exp(s - top), 0.0)
    total = jnp.sum(w, axis=0, keepdims=True)
    o = dot_tn(v, w.astype(jnp.bfloat16)) / total
    return heads_across(o).astype(jnp.bfloat16)


def three_parts(x):
    high = x.astype(jnp.bfloat16).astype(jnp.float32)
    rest = x - high
    middle = rest.astype(jnp.bfloat16).astype(jnp.float32)
    return high, middle, rest - middle


def member(w):
    return (w // SIDE % 2) * 2 + w % 2


def attend_kernel(
    wide_ref,
    span_ref,
    q0_ref,
    q1_ref,
    q2_ref,
    q3_ref,
    kv_ref,
    out_ref,
    list_ref,
    q_ref,
    top_ref,
    sum_ref,
    acc_ref,
):
    r = pl.program_id(0)
    w = wide_ref[0]
    y = w // SIDE
    x = w % SIDE
    j = r ^ member(w)

    @pl.when(r == 0)
    def _():
        for i, ref in enumerate((q0_ref, q1_ref, q2_ref, q3_ref)):
            q_ref[i] = ref[...]

    q_span = span_ref[((y // 2) * 2 + j // 2) * SIDE + (x // 2) * 2 + j % 2]
    qs = q_ref[r]
    cols = qs.shape[1]
    half = cols // 2
    count = jnp.int32(0)
    for i in range(kv_ref.shape[0]):
        span = span_ref[((i // 4) * 2 + y % 2) * SIDE + (i % 4) * 2 + x % 2]
        list_ref[count] = i
        count = count + jnp.where(span < q_span, 1, 0)
    for i in range(STEP):
        list_ref[count + i] = 0
    own = r == 0

    @pl.when(own)
    def _():
        kv = kv_ref[(y // 2) * 4 + x // 2]
        row = lax.broadcasted_iota(jnp.int32, (LONG_DEV, cols), 0)
        col = lax.broadcasted_iota(jnp.int32, (LONG_DEV, cols), 1)
        s = jnp.where(row <= col % LONG_DEV, dot(kv[:, :HEAD], qs), FAR)
        top = jnp.max(s, axis=0, keepdims=True)
        p = jnp.exp2((s - top) * SCALE2)
        top_ref[...] = top
        sum_ref[...] = jnp.sum(p, axis=0, keepdims=True)
        acc_ref[...] = dot(kv[:, HEAD:], p.astype(jnp.bfloat16))

    @pl.when(jnp.logical_not(own))
    def _():
        top_ref[...] = jnp.full(top_ref.shape, FAR, jnp.float32)
        sum_ref[...] = jnp.zeros(sum_ref.shape, jnp.float32)
        acc_ref[...] = jnp.zeros(acc_ref.shape, jnp.float32)

    def advance(t, last):
        ids = [list_ref[t * STEP + u] for u in range(STEP)]
        k = jnp.concatenate([kv_ref[i, :, :HEAD] for i in ids], axis=0)
        v = jnp.concatenate([kv_ref[i, :, HEAD:] for i in ids], axis=1)
        scores = [dot(k, qs[:, g * half : (g + 1) * half]) for g in range(2)]
        for g, s in enumerate(scores):
            if last:
                s = jnp.concatenate(
                    [
                        jnp.where(t * STEP + u < count, s[u * LONG_DEV : (u + 1) * LONG_DEV], FAR)
                        for u in range(STEP)
                    ],
                    axis=0,
                )
            at = slice(g * half, (g + 1) * half)
            old = top_ref[:, at]
            new = jnp.maximum(old, jnp.max(s, axis=0, keepdims=True))
            p = jnp.exp2((s - new) * SCALE2)
            factor = jnp.exp2((old - new) * SCALE2)
            top_ref[:, at] = new
            sum_ref[:, at] = sum_ref[:, at] * factor + jnp.sum(p, axis=0, keepdims=True)
            acc_ref[:, at] = acc_ref[:, at] * factor + dot(v, p.astype(jnp.bfloat16))

    def step(t, carry):
        advance(t, False)
        return carry

    lax.fori_loop(0, count // STEP, step, 0)

    @pl.when(count % STEP > 0)
    def _():
        advance(count // STEP, True)

    total = sum_ref[...]
    o = acc_ref[...] / jnp.where(total > 0.0, total, 1.0)
    out_ref[0, :HEAD] = o.astype(jnp.bfloat16)
    parts = (*three_parts(top_ref[...] * SCALE2), *three_parts(total))
    row = lax.broadcasted_iota(jnp.int32, (STATS, cols), 0)
    stats = jnp.zeros((STATS, cols), jnp.float32)
    for i, part in enumerate(parts):
        stats = jnp.where(row == i, part, stats)
    out_ref[0, HEAD:] = stats.astype(jnp.bfloat16)


def merged_rows(got_ref):
    tops, sums = [], []
    for j in range(got_ref.shape[0]):
        stats = got_ref[j, HEAD:].astype(jnp.float32)
        tops.append(stats[0:1] + stats[1:2] + stats[2:3])
        sums.append(stats[3:4] + stats[4:5] + stats[5:6])
    top = jnp.maximum(jnp.maximum(tops[0], tops[1]), jnp.maximum(tops[2], tops[3]))
    shares = [s * jnp.exp2(t - top) for s, t in zip(sums, tops)]
    total = (shares[0] + shares[1]) + (shares[2] + shares[3])
    o = got_ref[0, :HEAD].astype(jnp.float32) * (shares[0] / total)
    for j in range(1, 4):
        o = o + got_ref[j, :HEAD].astype(jnp.float32) * (shares[j] / total)
    return heads_across(o).astype(jnp.bfloat16)


def projector(make_rows):
    def kernel(core_ref, *refs):
        *inputs, weight_ref, send_ref, keep_ref, rows_ref = refs
        half = rows_ref.shape[0] // 2

        @pl.when(pl.program_id(0) == 0)
        def _():
            made = make_rows(*inputs)
            core = core_ref[0]
            for b in range(2):
                at = pl.multiple_of(jnp.where(core == b, half, 0), half)
                rows_ref[pl.ds(at, half), :] = made[b * half : (b + 1) * half]

        product = dot(rows_ref[...], weight_ref[...])
        rounded = product.astype(jnp.bfloat16)
        send_ref[...] = rounded[:half]
        keep_ref[...] = rounded[half:]

    return kernel


def whole(x):
    return pl.BlockSpec(x.shape, lambda *i: (0,) * x.ndim)


def project(make_rows, core, inputs, specs, weight, parts=1):
    cols, width = weight.shape
    width = width // parts
    half = LONG_DEV // 2
    block = 1024
    out = pl.BlockSpec((half, block), lambda i, c: (0, i))
    shape = jax.ShapeDtypeStruct((half, width), jnp.bfloat16)
    return pl.pallas_call(
        projector(make_rows),
        grid_spec=pltpu.PrefetchScalarGridSpec(
            num_scalar_prefetch=1,
            grid=(width // block,),
            in_specs=[
                *specs,
                pl.BlockSpec((cols, block), lambda i, c: (0, i)),
            ],
            out_specs=[out, out, pl.BlockSpec((2 * half, cols), lambda i, c: (0, 0))],
        ),
        out_shape=(shape, shape, jax.ShapeDtypeStruct((2 * half, cols), jnp.bfloat16)),
    )(core, *inputs, weight)


def rest_kernel(rows_ref, weight_ref, send_ref, keep_ref):
    rounded = dot(rows_ref[...], weight_ref[...]).astype(jnp.bfloat16)
    half = send_ref.shape[0]
    send_ref[...] = rounded[:half]
    keep_ref[...] = rounded[half:]


def project_rest(rows, weight):
    cols, width = weight.shape
    width = width // 2
    half = LONG_DEV // 2
    block = 1024
    first = width // block
    out = pl.BlockSpec((half, block), lambda i: (0, i))
    shape = jax.ShapeDtypeStruct((half, width), jnp.bfloat16)
    return pl.pallas_call(
        rest_kernel,
        grid=(width // block,),
        in_specs=[
            pl.BlockSpec((2 * half, cols), lambda i: (0, 0)),
            pl.BlockSpec((cols, block), lambda i: (0, i + first)),
        ],
        out_specs=[out, out],
        out_shape=(shape, shape),
        name="rest",
    )(rows, weight)


def pair_sum(a, b):
    return (a.astype(jnp.float32) + b.astype(jnp.float32)).astype(jnp.bfloat16)


def route_kernel(
    base0_ref, base1_ref, far0_ref, far1_ref, gain_ref, owner_ref, hidden_ref, out_ref, wide_ref
):
    hidden = jnp.concatenate(
        [
            base_ref[...] + far_ref[...].astype(jnp.float32)
            for base_ref, far_ref in ((base0_ref, far0_ref), (base1_ref, far1_ref))
        ],
        axis=1,
    ).astype(jnp.bfloat16)
    hidden_ref[...] = hidden
    h = hidden.astype(jnp.float32)
    mean = jnp.mean(h * h, axis=1, keepdims=True)
    normed = (h * lax.rsqrt(mean + 1e-05) * gain_ref[...].astype(jnp.float32)).astype(jnp.bfloat16)
    rows = h.shape[0]
    down = jnp.broadcast_to(owner_ref[...].astype(jnp.float32), (rows, HEAD))
    across = down.T[:rows]
    row = lax.broadcasted_iota(jnp.int32, (rows, rows), 0)
    col = lax.broadcasted_iota(jnp.int32, (rows, rows), 1)
    same = (down[:, :rows] == across) & (row < col)
    slot = jnp.sum(jnp.where(same, 1.0, 0.0), axis=0, keepdims=True)
    mine = across == row.astype(jnp.float32)
    owners = rows
    stride = out_ref.shape[0] // owners
    for s in range(2):
        pick = jnp.where(mine & (slot == float(s)), 1.0, 0.0).astype(jnp.bfloat16)
        placed = jnp.dot(pick, normed, preferred_element_type=jnp.float32)
        for t in range(stride // 2):
            wide_ref[pl.ds(s * (stride // 2) + t, owners, stride=stride), :] = placed[
                :, t * HEAD : (t + 1) * HEAD
            ]
    out_ref[...] = wide_ref[...].astype(jnp.bfloat16)


def in_vmem(x):
    return pltpu.with_memory_space_constraint(x, pltpu.VMEM)


def exchange(x, groups=None):
    return lax.all_to_all(x, "wide", 0, 0, tiled=True, axis_index_groups=groups)


def on_device(
    queries, key_rows, value_rows, residual, out_weight, norm_gain, span_map, segments, row_owner
):
    wide = lax.axis_index("wide").astype(jnp.int32).reshape(1)
    narrow = lax.axis_index("narrow").astype(jnp.int32).reshape(1)
    core = narrow & 1
    level = lax.shift_right_logical(narrow, jnp.ones_like(narrow))
    bf = jnp.bfloat16
    cols = queries.shape[1]
    width = out_weight.shape[1]
    vmem = pl.BlockSpec(memory_space=pltpu.VMEM)
    kv, qs = pl.pallas_call(
        prep_kernel,
        grid=(1,),
        in_specs=[
            pl.BlockSpec((LONG_DEV, x.shape[1]), lambda i: (0, 0))
            for x in (queries, key_rows, value_rows)
        ],
        out_specs=(
            pl.BlockSpec((16, LONG_DEV, 2 * HEAD), lambda i: (0, 0, 0)),
            pl.BlockSpec((LONG_DEV, cols), lambda i: (0, 0)),
        ),
        out_shape=(
            jax.ShapeDtypeStruct((16, LONG_DEV, 2 * HEAD), bf),
            jax.ShapeDtypeStruct((LONG_DEV, cols), bf),
        ),
        name="prep",
    )(queries, key_rows, value_rows)
    across = [(0, 1), (1, 0), (2, 3), (3, 2)]
    kv, qs, core_after = lax.optimization_barrier((kv, qs, core))
    kv = exchange(kv, KEY_GROUPS)
    devices = range(SIDE * SIDE)
    queries_by = [qs]
    for flip in FLIPS:
        queries_by.append(lax.ppermute(qs, "wide", [(i, i ^ flip) for i in devices]))
    short_in = (queries, key_rows, value_rows, segments)
    send, keep_short, _ = project(
        short_rows, core_after, short_in, [whole(x) for x in short_in], out_weight
    )
    near_short = lax.ppermute(send, "narrow", across)
    pair_short = pair_sum(keep_short, near_short)
    far_short = lax.ppermute(pair_short, "narrow", [(0, 2), (1, 3)])
    short = (keep_short.astype(jnp.float32) + near_short.astype(jnp.float32)) + far_short.astype(
        jnp.float32
    )
    parts = pl.pallas_call(
        attend_kernel,
        grid_spec=pltpu.PrefetchScalarGridSpec(
            num_scalar_prefetch=2,
            grid=(4,),
            in_specs=[vmem] * 5,
            out_specs=pl.BlockSpec(
                (1, HEAD + STATS, cols), lambda r, w, m: (r ^ member(w[0]), 0, 0)
            ),
            scratch_shapes=[
                pltpu.SMEM((16 + STEP,), jnp.int32),
                pltpu.VMEM((4, LONG_DEV, cols), bf),
                pltpu.VMEM((1, cols), jnp.float32),
                pltpu.VMEM((1, cols), jnp.float32),
                pltpu.VMEM((HEAD, cols), jnp.float32),
            ],
        ),
        out_shape=jax.ShapeDtypeStruct((4, HEAD + STATS, cols), bf),
        name="attend",
        compiler_params=ROOM,
    )(wide, span_map, *map(in_vmem, queries_by), in_vmem(kv))
    got = exchange(parts, QUERY_GROUPS)
    send, keep, placed = project(merged_rows, core, (in_vmem(got),), [vmem], out_weight, parts=2)
    near = lax.ppermute(send, "narrow", across)
    send_rest, keep_rest = project_rest(placed, out_weight)
    near_rest = lax.ppermute(send_rest, "narrow", across)
    bases, fars = [], []
    for part, (k, n) in enumerate(((keep, near), (keep_rest, near_rest))):
        pair, k, n = lax.optimization_barrier((pair_sum(k, n), k, n))
        fars.append(lax.ppermute(pair, "narrow", [(2, 0), (3, 1)]))
        at = slice(part * width // 2, (part + 1) * width // 2)
        long = k.astype(jnp.float32) + n.astype(jnp.float32)
        bases.append(
            residual[:, at].astype(jnp.float32) + jnp.where(level[0] == 0, long, short[:, at])
        )
    rows = residual.shape[0]
    owners = 64
    tiles = 2 * width // HEAD
    hidden, outgoing = pl.pallas_call(
        route_kernel,
        in_specs=[vmem] * 6,
        out_shape=(
            jax.ShapeDtypeStruct((rows, width), bf),
            jax.ShapeDtypeStruct((owners * tiles, HEAD), bf),
        ),
        scratch_shapes=[pltpu.VMEM((owners * tiles, HEAD), jnp.float32)],
        name="route",
        compiler_params=ROOM,
    )(*map(in_vmem, bases), *map(in_vmem, fars), norm_gain.reshape(1, width), row_owner)
    arrived = exchange(outgoing.reshape(owners, tiles, HEAD))
    return (hidden, arrived.reshape(1, 1, owners, 2, width))


def solution(mesh):
    placed = (
        P(("rep", "wide"), "narrow"),
        P(("rep", "wide"), "narrow"),
        P(("rep", "wide"), "narrow"),
        P(("rep", "wide", "narrow"), None),
        P("narrow", None),
        P(),
        P(),
        P(("rep", "wide"), None),
        P(("rep", "wide", "narrow"), None),
    )
    return jax.shard_map(
        on_device,
        mesh=mesh,
        in_specs=placed,
        out_specs=(
            P(("rep", "wide", "narrow"), None),
            P(("rep", "wide"), "narrow", None, None, None),
        ),
        check_vma=False,
    )
```
